256 devices in a mesh: tm: 32 (over x_lo, z, core), space: 8 (over y, x_hi).
Axes of the slice: x: 4 (x_hi: 2, x_lo: 2; x = x_hi * 2 + x_lo), y: 4, z: 8, core: 2. Of those that a mesh axis runs over, the one named last changes fastest.
Arguments:
- forcing: float32 [32, 32, 128, 128], P('tm', 'space'), may hold values from -6 to 6
- initial: float32 [32, 128, 128], P('space'), may hold values from -6 to 6
- coupling: float32 [32, 128, 128], P('space'), may hold values from 0.3 to 3
- velocity: float32 [3, 32, 128, 128], P(None, 'space'), may hold values from -0.9 to 0.9
Outputs:
- iterate: float32 [32, 32, 128, 128], P('tm', 'space')
The draws below stay inside these ranges and needn't reach their ends.
All inputs are finite; a program needn't handle non-finite values.
Results may differ from the reference program's by a relative error of at most 0.0003.
Values sent between devices are 32-bit elements; how exact they have to be, the bound alone decides.
A program may use at most 64 MiB of HBM per device.

```python
import math
import jax
import jax.numpy as jnp
from jax import lax

NY = 128
NX = 128
ITERS = 2
SWEEPS = 8
NT = 32
NZ = 32


def level_of(stream_key, shape, cuts, low, top_value):
    level = 1.0
    for axis_at, parts in cuts:
        draws = jax.random.uniform(jax.random.fold_in(jax.random.fold_in(stream_key, 6), axis_at), (parts,), jnp.float32, low / len(cuts), top_value / len(cuts))
        level = level * jnp.repeat(jnp.exp(draws), shape[axis_at] // parts).reshape((-1,) + (1,) * (len(shape) - 1 - axis_at))
    return level


def gaussian(key, dims, width, reach, shards=(), kind=jnp.bfloat16):
    array = width * jax.random.normal(key, dims, jnp.float32)
    if shards:
        array = array * level_of(key, dims, shards, -0.22, 0.18)
    return jnp.clip(array, -reach, reach).astype(kind)


def setup_inputs(seed: int = 0) -> dict:
    arg_keys = jax.random.split(jax.random.key(seed), 5)
    forcing = gaussian(arg_keys[0], (NT, NZ, NY, NX), 1.0, 6.0, ((0, 32), (1, 8)), jnp.float32)
    initial = gaussian(arg_keys[1], (NZ, NY, NX), 1.0, 6.0, ((0, 8),), jnp.float32)
    coupling = jnp.clip(jnp.exp(math.log(3.0) - 2.3025851 * jax.random.uniform(arg_keys[2], (NZ, NY, NX), jnp.float32) ** level_of(arg_keys[2], (NZ, NY, NX), ((0, 8),), -0.2, 0.2)), 0.3, 3.0)
    velocity = jnp.clip(jax.random.uniform(arg_keys[3], (3, NZ, NY, NX), jnp.float32, -0.9, 0.9) * level_of(arg_keys[3], (3, NZ, NY, NX), ((1, 8),), -0.4, 0.0), -0.9, 0.9)
    return dict(forcing=forcing, initial=initial, coupling=coupling, velocity=velocity)


wrap_alpha = 0.1


def padded(field):
    widths = [(0, 0)] * (field.ndim - 3) + [(1, 1)] * 3
    return jnp.pad(field, widths)


def coupled(extended, coupling, advect):
    total = (coupling - advect[0]) * extended[..., 2:, 1:-1, 1:-1] + (coupling + advect[0]) * extended[..., :-2, 1:-1, 1:-1]
    total = total + (coupling - advect[1]) * extended[..., 1:-1, 2:, 1:-1] + (coupling + advect[1]) * extended[..., 1:-1, :-2, 1:-1]
    total = total + (coupling - advect[2]) * extended[..., 1:-1, 1:-1, 2:] + (coupling + advect[2]) * extended[..., 1:-1, 1:-1, :-2]
    return total


def tables(total_steps):
    indices = jnp.arange(total_steps, dtype=jnp.int32)
    products = (indices[:, None] * indices[None, :]) % total_steps
    angles = products.astype(jnp.float32) * (2.0 * math.pi / total_steps)
    return jnp.cos(angles), jnp.sin(angles)


def matmul(table, columns):
    return jnp.dot(table, columns, preferred_element_type=jnp.float32, precision=lax.Precision.HIGHEST)


def reference(forcing, initial, coupling, velocity):
    total_steps = forcing.shape[0]
    shape = forcing.shape
    advect = coupling[None] * velocity
    cosine, sine_table = tables(total_steps)
    steps_float = jnp.arange(total_steps, dtype=jnp.float32)
    time_weight = jnp.exp(math.log(wrap_alpha) * steps_float / total_steps)[:, None, None, None]
    radius = math.exp(math.log(wrap_alpha) / total_steps)
    angles = steps_float * (2.0 * math.pi / total_steps)
    shift_re = radius * jnp.cos(angles)
    shift_im = radius * jnp.sin(angles)
    iterate = jnp.broadcast_to(initial, shape).astype(jnp.float32)

    def solve(pieces):
        source_re, source_im, freq_re, freq_im = pieces
        diag_re = 1.0 + 6.0 * coupling - freq_re
        diag_im = freq_im
        modulus = diag_re * diag_re + diag_im * diag_im
        value_re = (source_re * diag_re + source_im * diag_im) / modulus
        value_im = (source_im * diag_re - source_re * diag_im) / modulus
        for sweep in range(SWEEPS):
            sum_re = source_re + coupled(padded(value_re), coupling, advect)
            sum_im = source_im + coupled(padded(value_im), coupling, advect)
            value_re = (sum_re * diag_re + sum_im * diag_im) / modulus
            value_im = (sum_im * diag_re - sum_re * diag_im) / modulus
        return value_re, value_im

    for repeat in range(ITERS):
        previous = jnp.concatenate([initial[None], iterate[:-1]], axis=0)
        residual = forcing - ((1.0 + 6.0 * coupling) * iterate - coupled(padded(iterate), coupling, advect)) + previous
        columns = (residual * time_weight).reshape(total_steps, -1)
        spec_re = matmul(cosine, columns).reshape(shape)
        spec_im = (-matmul(sine_table, columns)).reshape(shape)
        value_re, value_im = lax.map(solve, (spec_re, spec_im, shift_re, shift_im))
        inverse_part = (matmul(cosine, value_re.reshape(total_steps, -1)) - matmul(sine_table, value_im.reshape(total_steps, -1))) / total_steps
        iterate = iterate + inverse_part.reshape(shape) / time_weight
    return iterate
```

```python
import functools
import math

import jax
import jax.numpy as jnp
import numpy as np
from jax import lax
from jax.experimental import pallas as pl
from jax.experimental.pallas import tpu as pltpu
from jax.sharding import PartitionSpec as P

STEPS = 32
ALPHA = 0.1
RHO = ALPHA ** (1.0 / STEPS)
GAMMA = [ALPHA ** (n / STEPS) for n in range(STEPS)]
GROUPS = 2
MESH = pl.DeviceIdType.MESH
F32 = jnp.float32


def real_fft(xs):
    size = len(xs)
    if size == 2:
        return [xs[0] + xs[1], xs[0] - xs[1]], [None, None]
    even_re, even_im = real_fft(xs[0::2])
    odd_re, odd_im = real_fft(xs[1::2])
    half, quarter = size // 2, size // 4
    re, im = [None] * (half + 1), [None] * (half + 1)
    re[0], re[half] = even_re[0] + odd_re[0], even_re[0] - odd_re[0]
    for j in range(1, quarter):
        c, s = math.cos(2 * math.pi * j / size), math.sin(2 * math.pi * j / size)
        t_re = c * odd_re[j] + s * odd_im[j]
        t_im = c * odd_im[j] - s * odd_re[j]
        re[j], im[j] = even_re[j] + t_re, even_im[j] + t_im
        re[half - j], im[half - j] = even_re[j] - t_re, t_im - even_im[j]
    re[quarter], im[quarter] = even_re[quarter], -odd_re[quarter]
    return re, im


def real_ifft(re, im):
    half = len(re) - 1
    size = 2 * half
    if size == 2:
        return [re[0] + re[1], re[0] - re[1]]
    quarter = size // 4
    even_re, even_im = [None] * (quarter + 1), [None] * (quarter + 1)
    odd_re, odd_im = [None] * (quarter + 1), [None] * (quarter + 1)
    even_re[0], odd_re[0] = re[0] + re[half], re[0] - re[half]
    for j in range(1, quarter):
        c, s = math.cos(2 * math.pi * j / size), math.sin(2 * math.pi * j / size)
        even_re[j], even_im[j] = re[j] + re[half - j], im[j] - im[half - j]
        t_re, t_im = re[j] - re[half - j], im[j] + im[half - j]
        odd_re[j], odd_im[j] = c * t_re - s * t_im, c * t_im + s * t_re
    even_re[quarter], odd_re[quarter] = 2.0 * re[quarter], -2.0 * im[quarter]
    even = real_ifft(even_re, even_im)
    odd = real_ifft(odd_re, odd_im)
    return [(even, odd)[n % 2][n // 2] for n in range(size)]


def unit_tables():
    slots = STEPS // 2
    j = np.arange(slots)
    theta = 2 * np.pi * j / STEPS
    n = np.arange(STEPS)
    gamma = np.array(GAMMA)
    angle = 2 * np.pi * ((j[:, None] * n[None, :]) % STEPS) / STEPS
    shift_re = RHO * np.cos(theta)
    shift_re_im = shift_re.copy()
    shift_re_im[0] = -RHO
    shift_im = RHO * np.sin(theta)
    shift_im[0] = 0.0
    const_re = (np.cos(angle) * gamma).sum(1)
    const_im = -(np.sin(angle) * gamma).sum(1)
    const_im[0] = (gamma * (-1.0) ** n).sum()
    last = 2 * np.pi * ((j * (STEPS - 1)) % STEPS) / STEPS
    last_re = 2 * np.cos(last) * RHO / STEPS
    last_im = -2 * np.sin(last) * RHO / STEPS
    last_re[0] = RHO / STEPS
    last_im[0] = -RHO / STEPS
    delta_re = np.ones(slots)
    delta_im = np.zeros(slots)
    delta_im[0] = 1.0
    rows = np.stack(
        [shift_re, shift_re_im, shift_im, const_re, const_im, last_re, last_im, delta_re, delta_im]
    )
    rows = rows.reshape(9, GROUPS, 8).transpose(1, 0, 2)
    return np.ascontiguousarray(np.broadcast_to(rows[..., None], (GROUPS, 9, 8, 128))).astype(np.float32)


def unit_of(j, imaginary):
    if j == STEPS // 2:
        j, imaginary = 0, True
    return (j // 8) * 16 + (8 if imaginary else 0) + j % 8


def device_at(m, zz):
    r, along = lax.rem(m, 4), lax.div(m, 4)
    x = r + lax.rem(along, 2) * (3 - 2 * r)
    return (
        lax.rem(x, 2) * 16 + along * 2 + lax.rem(zz, 2),
        lax.div(zz, 2) * 2 + lax.div(x, 2),
    )


def kernel(
    forcing,
    initial,
    coupling,
    velocity,
    table_in,
    out,
    slab,
    params,
    table,
    packed,
    times,
    spread,
    back,
    gathered,
    pack_params,
    own_params,
    near,
    coef,
    diag,
    d,
    total,
    wrap,
    load_sem,
    out_send,
    out_recv,
    back_send,
    back_recv,
    param_send,
    param_recv,
    near_send,
    near_recv,
    halo_send,
    halo_recv,
):
    me_t, me_s = lax.axis_index("tm"), lax.axis_index("space")
    core, along = lax.rem(me_t, 2), lax.rem(lax.div(me_t, 2), 8)
    row, x_hi = lax.div(me_s, 2), lax.rem(me_s, 2)
    x = 2 * x_hi + lax.div(me_t, 16)
    r = x + lax.rem(along, 2) * (3 - 2 * x)
    m = along * 4 + r
    zz = row * 2 + core
    swap = lax.rem(core + x_hi, 2)
    target = m + swap * (3 - 2 * r)

    loads = [
        pltpu.make_async_copy(forcing, slab, load_sem.at[0]),
        pltpu.make_async_copy(table_in, table, load_sem.at[1]),
    ]
    window = pl.ds(pl.multiple_of(lax.div(target, 2) * 8, 8), 8)
    param_loads = [
        pltpu.make_async_copy(coupling.at[:, window], params.at[0], load_sem.at[2]),
        pltpu.make_async_copy(velocity.at[:, :, window], params.at[pl.ds(1, 3)], load_sem.at[3]),
        pltpu.make_async_copy(initial.at[:, window], params.at[4], load_sem.at[4]),
    ]
    for load in loads + param_loads:
        load.start()

    zeros = jnp.zeros((16, 128), F32)
    for g in range(GROUPS):
        for parity in range(2):
            for i in range(4):
                for z, y in ((0, i + 1), (5, i + 1), (i + 1, 0), (i + 1, 5)):
                    d[g, parity, z, y] = zeros
    for side in range(4):
        near[side, 4] = zeros

    barrier = pltpu.get_barrier_semaphore()

    def greet(i, carry):
        t, b = lax.div(i, 2), lax.rem(i, 2)

        @pl.when(jnp.logical_or(t != me_t, b != x_hi))
        def _():
            pl.semaphore_signal(barrier, inc=1, device_id=(t, row * 2 + b), device_id_type=MESH)

        return carry

    lax.fori_loop(0, 64, greet, 0)
    side_device = [
        device_at(m - 1, zz),
        device_at(m + 1, zz),
        device_at(m, zz - 1),
        device_at(m, zz + 1),
    ]
    has = [m > 0, m < 31, zz > 0, zz < 7]
    far_z = [jnp.logical_and(core == 0, row > 0), jnp.logical_and(core == 1, row < 3)]
    for side in (2, 3):

        @pl.when(far_z[side - 2])
        def _():
            pl.semaphore_signal(barrier, inc=1, device_id=side_device[side], device_id_type=MESH)

    low = lax.broadcasted_iota(jnp.int32, (8, 128), 0) < 4
    loads[0].wait()

    def pack(t, carry):
        rows = pl.ds(pl.multiple_of(t * 8, 8), 8)
        v = [slab[z, rows] for z in range(4)]
        w = [pltpu.roll(a, 4, 0) for a in v]
        packed[2 * t, 0:8] = jnp.where(low, v[0], w[1])
        packed[2 * t, 8:16] = jnp.where(low, v[2], w[3])
        packed[2 * t + 1, 0:8] = jnp.where(low, w[0], v[1])
        packed[2 * t + 1, 8:16] = jnp.where(low, w[2], v[3])
        return carry

    lax.fori_loop(0, 16, pack, 0)
    far_count = jnp.logical_or(far_z[0], far_z[1]).astype(jnp.int32)
    pl.semaphore_wait(barrier, 63 + far_count)

    def out_copy(i):
        return pltpu.make_async_remote_copy(
            src_ref=packed.at[i],
            dst_ref=times.at[me_t],
            send_sem=out_send.at[i],
            recv_sem=out_recv.at[me_t],
            device_id=device_at(i, row * 2 + x_hi),
            device_id_type=MESH,
        )

    def is_self(i):
        return jnp.logical_and(i == m, swap == 0)

    def out_start(k, carry):
        i = lax.rem(m + 1 + k, 32)

        @pl.when(jnp.logical_not(is_self(i)))
        def _():
            out_copy(i).start()

        return carry

    lax.fori_loop(0, 32, out_start, 0)

    @pl.when(swap == 0)
    def _():
        times[me_t] = packed[m]

    for load in param_loads:
        load.wait()
    odd = lax.rem(target, 2) == 1
    for f in range(5):
        v = [params[f, z] for z in range(4)]
        w = [pltpu.roll(a, 4, 0) for a in v]
        v, w = [jnp.where(odd, b, a) for a, b in zip(v, w)], [jnp.where(odd, a, b) for a, b in zip(v, w)]
        pack_params[f, 0:8] = jnp.where(low, v[0], w[1])
        pack_params[f, 8:16] = jnp.where(low, v[2], w[3])
    param_copy = pltpu.make_async_remote_copy(
        src_ref=pack_params,
        dst_ref=own_params,
        send_sem=param_send,
        recv_sem=param_recv,
        device_id=device_at(target, row * 2 + 1 - core),
        device_id_type=MESH,
    )
    @pl.when(swap == 1)
    def _():
        param_copy.start()
        param_copy.wait()

    @pl.when(swap == 0)
    def _():
        own_params[...] = pack_params[...]

    def near_copy(side):
        return pltpu.make_async_remote_copy(
            src_ref=own_params.at[4],
            dst_ref=near.at[side, 4],
            send_sem=near_send.at[side],
            recv_sem=near_recv.at[side],
            device_id=side_device[side],
            device_id_type=MESH,
        )

    opposite = (1, 0, 3, 2)
    for side in range(4):

        @pl.when(has[side])
        def _():
            near_copy(side).start()

    c = own_params[0]
    lane = lax.broadcasted_iota(jnp.int32, (16, 128), 1)
    sub = lax.broadcasted_iota(jnp.int32, (16, 128), 0)
    flow = [c * own_params[1 + k] for k in range(3)]
    coefs = [
        c - flow[0],
        c + flow[0],
        c - flow[1],
        c + flow[1],
        jnp.where(lane == 127, 0.0, c - flow[2]),
        jnp.where(lane == 0, 0.0, c + flow[2]),
    ]
    for p in range(16):
        for k in range(6):
            coef[p, k] = jnp.broadcast_to(coefs[k][p : p + 1], (8, 128))
    loads[1].wait()
    middle = 1.0 + 6.0 * c
    for p in range(16):
        mid = jnp.broadcast_to(middle[p : p + 1], (8, 128))
        for g in range(GROUPS):
            d_re, d_im, s_im = mid - table[g, 0], mid - table[g, 1], table[g, 2]
            inv = 1.0 / (d_re * d_re + s_im * s_im)
            diag[g, p, 0] = d_re * inv
            diag[g, p, 1] = d_im / (d_im * d_im + s_im * s_im)
            diag[g, p, 2] = s_im * inv
    for side in range(4):

        @pl.when(has[side])
        def _():
            near_copy(side).wait_send()

        @pl.when(has[opposite[side]])
        def _():
            near_copy(side).wait_recv()

    own = own_params[4]
    after_y, before_y, after_z, before_z = [near[side, 4] for side in range(4)]
    step = lax.rem(sub, 4)
    summed = coefs[0] * jnp.where(sub < 12, pltpu.roll(own, 12, 0), pltpu.roll(after_z, 12, 0))
    summed += coefs[1] * jnp.where(sub >= 4, pltpu.roll(own, 4, 0), pltpu.roll(before_z, 4, 0))
    summed += coefs[2] * jnp.where(step < 3, pltpu.roll(own, 15, 0), pltpu.roll(after_y, 3, 0))
    summed += coefs[3] * jnp.where(step > 0, pltpu.roll(own, 1, 0), pltpu.roll(before_y, 13, 0))
    summed += coefs[4] * pltpu.roll(own, 127, 1) + coefs[5] * pltpu.roll(own, 1, 1)
    source = summed - 6.0 * c * own

    def out_finish(i, carry):
        @pl.when(jnp.logical_not(is_self(i)))
        def _():
            out_copy(i).wait_send()

        @pl.when(jnp.logical_or(i != me_t, swap == 1))
        def _():
            pltpu.make_async_remote_copy(
                src_ref=packed.at[i],
                dst_ref=times.at[i],
                send_sem=out_send.at[i],
                recv_sem=out_recv.at[i],
                device_id=(me_t, me_s),
                device_id_type=MESH,
            ).wait_recv()

        return carry

    lax.fori_loop(0, 32, out_finish, 0)

    def transform(h, carry):
        rows = pl.ds(pl.multiple_of(h * 8, 8), 8)
        re, im = real_fft([GAMMA[n] * times[n, rows] for n in range(32)])
        for j in range(17):
            spread[pl.ds(h * 256 + unit_of(j, False), 8, stride=32), :] = re[j]
            if im[j] is not None:
                spread[pl.ds(h * 256 + unit_of(j, True), 8, stride=32), :] = im[j]
        return carry

    lax.fori_loop(0, 2, transform, 0)

    def halo_copy(g, parity, side):
        if side < 2:
            src, dst = (1, 5) if side == 0 else (4, 0)
            src_ref = d.at[g, parity, pl.ds(1, 4), src]
            dst_ref = d.at[g, parity, pl.ds(1, 4), dst]
        else:
            src, dst = (1, 5) if side == 2 else (4, 0)
            src_ref = d.at[g, parity, src, pl.ds(1, 4)]
            dst_ref = d.at[g, parity, dst, pl.ds(1, 4)]
        return pltpu.make_async_remote_copy(
            src_ref=src_ref,
            dst_ref=dst_ref,
            send_sem=halo_send.at[g, parity, side],
            recv_sem=halo_recv.at[g, parity, side],
            device_id=side_device[side],
            device_id_type=MESH,
        )

    def halo_start(g, parity):
        for side in range(4):

            @pl.when(has[side])
            def _():
                halo_copy(g, parity, side).start()

    def halo_wait(g, parity):
        for side in range(4):

            @pl.when(has[side])
            def _():
                halo_copy(g, parity, side).wait_send()

            @pl.when(has[opposite[side]])
            def _():
                halo_copy(g, parity, side).wait_recv()

    def divide(g, p, s_re, s_im):
        a_re, a_im, b = diag[g, p, 0], diag[g, p, 1], diag[g, p, 2]
        return a_re * s_re + b * s_im, a_im * s_im - b * s_re

    for g in range(GROUPS):
        for p in range(16):
            z, y = p // 4, p % 4
            base = jnp.broadcast_to(source[p : p + 1], (8, 128))
            first = p * 32 + g * 16
            v_re, v_im = divide(
                g,
                p,
                spread[first : first + 8] + table[g, 3] * base,
                spread[first + 8 : first + 16] + table[g, 4] * base,
            )
            d[g, 0, z + 1, y + 1, 0:8] = v_re
            d[g, 0, z + 1, y + 1, 8:16] = v_im
            total[first : first + 8] = v_re
            total[first + 8 : first + 16] = v_im
        halo_start(g, 0)

    def sweep(g, parity, wrapped, send):
        halo_wait(g, parity)
        for p in range(16):
            z, y = p // 4 + 1, p % 4 + 1
            result = []
            for half in range(2):
                rows = slice(half * 8, half * 8 + 8)
                here = d[g, parity, z, y, rows]
                s = coef[p, 0] * d[g, parity, z + 1, y, rows]
                s += coef[p, 1] * d[g, parity, z - 1, y, rows]
                s += coef[p, 2] * d[g, parity, z, y + 1, rows]
                s += coef[p, 3] * d[g, parity, z, y - 1, rows]
                s += coef[p, 4] * pltpu.roll(here, 127, 1)
                s += coef[p, 5] * pltpu.roll(here, 1, 1)
                if wrapped:
                    s -= table[g, 7 + half] * wrap[p]
                result.append(s)
            v_re, v_im = divide(g, p, *result)
            d[g, 1 - parity, z, y, 0:8] = v_re
            d[g, 1 - parity, z, y, 8:16] = v_im
            first = p * 32 + g * 16
            total[first : first + 8] += v_re
            total[first + 8 : first + 16] += v_im
        if send:
            halo_start(g, 1 - parity)

    def both(k, carry):
        for g in range(GROUPS):
            sweep(g, lax.rem(k + 1, 2), False, True)
        return carry

    lax.fori_loop(1, 9, both, 0)
    for p in range(16):
        s = jnp.zeros((8, 128), F32)
        for g in range(GROUPS):
            first = p * 32 + g * 16
            s += table[g, 5] * total[first : first + 8]
            s += table[g, 6] * total[first + 8 : first + 16]
        wrap[p] = jnp.broadcast_to(jnp.sum(s, axis=0, keepdims=True), (8, 128))
    for g in range(GROUPS):
        sweep(g, 0, True, True)
    lax.fori_loop(10, 17, both, 0)
    for g in range(GROUPS):
        sweep(g, 0, False, False)

    def restore(h, carry):
        rows = pl.ds(pl.multiple_of(h * 8, 8), 8)
        re, im = [None] * 17, [None] * 17
        for j in range(17):
            re[j] = total[pl.ds(h * 256 + unit_of(j, False), 8, stride=32), :]
            if 0 < j < 16:
                im[j] = total[pl.ds(h * 256 + unit_of(j, True), 8, stride=32), :]
        for n, value in enumerate(real_ifft(re, im)):
            back[n, rows] = value * (1.0 / (STEPS * GAMMA[n]))
        return carry

    lax.fori_loop(0, 2, restore, 0)

    def back_copy(i):
        return pltpu.make_async_remote_copy(
            src_ref=back.at[i],
            dst_ref=gathered.at[m],
            send_sem=back_send.at[i],
            recv_sem=back_recv.at[m],
            device_id=(i, row * 2 + core),
            device_id_type=MESH,
        )

    def is_own(i):
        return jnp.logical_and(i == me_t, swap == 0)

    def back_start(k, carry):
        i = lax.rem(me_t + 1 + k, 32)

        @pl.when(jnp.logical_not(is_own(i)))
        def _():
            back_copy(i).start()

        return carry

    lax.fori_loop(0, 32, back_start, 0)

    @pl.when(swap == 0)
    def _():
        gathered[m] = back[me_t]

    def back_finish(i, carry):
        @pl.when(jnp.logical_not(is_own(i)))
        def _():
            back_copy(i).wait_send()

        @pl.when(jnp.logical_not(is_self(i)))
        def _():
            pltpu.make_async_remote_copy(
                src_ref=back.at[i],
                dst_ref=gathered.at[i],
                send_sem=back_send.at[i],
                recv_sem=back_recv.at[i],
                device_id=(me_t, me_s),
                device_id_type=MESH,
            ).wait_recv()

        return carry

    lax.fori_loop(0, 32, back_finish, 0)

    def unpack(t, carry):
        rows = pl.ds(pl.multiple_of(t * 8, 8), 8)
        p = [gathered[2 * t, 0:8], gathered[2 * t, 8:16]]
        q = [gathered[2 * t + 1, 0:8], gathered[2 * t + 1, 8:16]]
        for i in range(2):
            out[2 * i, rows] = jnp.where(low, p[i], pltpu.roll(q[i], 4, 0))
            out[2 * i + 1, rows] = jnp.where(low, pltpu.roll(p[i], 4, 0), q[i])
        return carry

    lax.fori_loop(0, 16, unpack, 0)


def body(forcing, initial, coupling, velocity):
    local = forcing.shape[1:]
    table = jnp.asarray(unit_tables())
    hbm = pl.BlockSpec(memory_space=pl.ANY)
    dma = pltpu.SemaphoreType.DMA
    correction = pl.pallas_call(
        kernel,
        out_shape=jax.ShapeDtypeStruct(local, F32),
        in_specs=[hbm] * 5,
        out_specs=pl.BlockSpec(memory_space=pltpu.VMEM),
        scratch_shapes=[
            pltpu.VMEM(local, F32),
            pltpu.VMEM((5, 4, 8, 128), F32),
            pltpu.VMEM((GROUPS, 9, 8, 128), F32),
            pltpu.VMEM((32, 16, 128), F32),
            pltpu.VMEM((32, 16, 128), F32),
            pltpu.VMEM((512, 128), F32),
            pltpu.VMEM((32, 16, 128), F32),
            pltpu.VMEM((32, 16, 128), F32),
            pltpu.VMEM((5, 16, 128), F32),
            pltpu.VMEM((5, 16, 128), F32),
            pltpu.VMEM((4, 5, 16, 128), F32),
            pltpu.VMEM((16, 6, 8, 128), F32),
            pltpu.VMEM((GROUPS, 16, 3, 8, 128), F32),
            pltpu.VMEM((GROUPS, 2, 6, 6, 16, 128), F32),
            pltpu.VMEM((512, 128), F32),
            pltpu.VMEM((16, 8, 128), F32),
            dma((5,)),
            dma((32,)),
            dma((32,)),
            dma((32,)),
            dma((32,)),
            dma,
            dma,
            dma((4,)),
            dma((4,)),
            dma((GROUPS, 2, 4)),
            dma((GROUPS, 2, 4)),
        ],
        compiler_params=pltpu.CompilerParams(collective_id=0, has_side_effects=True),
    )(forcing[0], initial, coupling, velocity, table)
    return (initial + correction)[None]


def solution(mesh):
    return jax.shard_map(
        body,
        mesh=mesh,
        in_specs=(
            P("tm", "space", None, None),
            P("space", None, None),
            P("space", None, None),
            P(None, "space", None, None),
        ),
        out_specs=P("tm", "space", None, None),
        check_vma=False,
    )
```

```python
import functools
import math

import jax
import jax.numpy as jnp
import numpy as np
from jax import lax
from jax.experimental import pallas as pl
from jax.experimental.pallas import tpu as pltpu
from jax.sharding import PartitionSpec as P

STEPS = 32
ALPHA = 0.1
RHO = ALPHA ** (1.0 / STEPS)
GAMMA = [ALPHA ** (n / STEPS) for n in range(STEPS)]
GROUPS = 4
SLOTS = STEPS // 2 // GROUPS
MESH = pl.DeviceIdType.MESH
F32 = jnp.float32


def real_fft(xs):
    size = len(xs)
    if size == 2:
        return [xs[0] + xs[1], xs[0] - xs[1]], [None, None]
    even_re, even_im = real_fft(xs[0::2])
    odd_re, odd_im = real_fft(xs[1::2])
    half, quarter = size // 2, size // 4
    re, im = [None] * (half + 1), [None] * (half + 1)
    re[0], re[half] = even_re[0] + odd_re[0], even_re[0] - odd_re[0]
    for j in range(1, quarter):
        c, s = math.cos(2 * math.pi * j / size), math.sin(2 * math.pi * j / size)
        t_re = c * odd_re[j] + s * odd_im[j]
        t_im = c * odd_im[j] - s * odd_re[j]
        re[j], im[j] = even_re[j] + t_re, even_im[j] + t_im
        re[half - j], im[half - j] = even_re[j] - t_re, t_im - even_im[j]
    re[quarter], im[quarter] = even_re[quarter], -odd_re[quarter]
    return re, im


def real_ifft(re, im):
    half = len(re) - 1
    size = 2 * half
    if size == 2:
        return [re[0] + re[1], re[0] - re[1]]
    quarter = size // 4
    even_re, even_im = [None] * (quarter + 1), [None] * (quarter + 1)
    odd_re, odd_im = [None] * (quarter + 1), [None] * (quarter + 1)
    even_re[0], odd_re[0] = re[0] + re[half], re[0] - re[half]
    for j in range(1, quarter):
        c, s = math.cos(2 * math.pi * j / size), math.sin(2 * math.pi * j / size)
        even_re[j], even_im[j] = re[j] + re[half - j], im[j] - im[half - j]
        t_re, t_im = re[j] - re[half - j], im[j] + im[half - j]
        odd_re[j], odd_im[j] = c * t_re - s * t_im, c * t_im + s * t_re
    even_re[quarter], odd_re[quarter] = 2.0 * re[quarter], -2.0 * im[quarter]
    even = real_ifft(even_re, even_im)
    odd = real_ifft(odd_re, odd_im)
    return [(even, odd)[n % 2][n // 2] for n in range(size)]


def unit_tables():
    slots = STEPS // 2
    j = np.arange(slots)
    theta = 2 * np.pi * j / STEPS
    n = np.arange(STEPS)
    gamma = np.array(GAMMA)
    angle = 2 * np.pi * ((j[:, None] * n[None, :]) % STEPS) / STEPS
    last = 2 * np.pi * ((j * (STEPS - 1)) % STEPS) / STEPS
    re = np.stack(
        [
            RHO * np.cos(theta),
            RHO * np.sin(theta),
            (np.cos(angle) * gamma).sum(1),
            2 * np.cos(last) * RHO / STEPS,
            np.ones(slots),
        ]
    )
    im = np.stack(
        [
            RHO * np.cos(theta),
            -RHO * np.sin(theta),
            -(np.sin(angle) * gamma).sum(1),
            -2 * np.sin(last) * RHO / STEPS,
            np.zeros(slots),
        ]
    )
    re[1, 0] = im[1, 0] = 0.0
    re[3, 0] = RHO / STEPS
    im[:, 0] = [-RHO, 0.0, (gamma * (-1.0) ** n).sum(), -RHO / STEPS, 1.0]
    rows = np.concatenate([re.reshape(5, GROUPS, SLOTS), im.reshape(5, GROUPS, SLOTS)], axis=2)
    rows = rows.transpose(1, 0, 2)[..., None]
    return np.ascontiguousarray(np.broadcast_to(rows, (GROUPS, 5, 8, 128))).astype(np.float32)


def unit_of(j, imaginary):
    if j == STEPS // 2:
        j, imaginary = 0, True
    return (j // SLOTS) * 8 + (SLOTS if imaginary else 0) + j % SLOTS


def device_at(m, zz):
    r, along = lax.rem(m, 4), lax.div(m, 4)
    x = r + lax.rem(along, 2) * (3 - 2 * r)
    return (
        lax.rem(x, 2) * 16 + along * 2 + lax.rem(zz, 2),
        lax.div(zz, 2) * 2 + lax.div(x, 2),
    )


def kernel(
    forcing,
    initial,
    coupling,
    velocity,
    table_in,
    out,
    slab,
    params,
    table,
    packed,
    times,
    spread,
    back,
    gathered,
    pack_params,
    own_params,
    near,
    coef,
    diag,
    d,
    middle_d,
    total,
    wrap,
    load_sem,
    out_send,
    out_recv,
    back_send,
    back_recv,
    param_send,
    param_recv,
    near_send,
    near_recv,
    halo_send,
    halo_recv,
):
    me_t, me_s = lax.axis_index("tm"), lax.axis_index("space")
    core, along = lax.rem(me_t, 2), lax.rem(lax.div(me_t, 2), 8)
    row, x_hi = lax.div(me_s, 2), lax.rem(me_s, 2)
    x = 2 * x_hi + lax.div(me_t, 16)
    r = x + lax.rem(along, 2) * (3 - 2 * x)
    m = along * 4 + r
    zz = row * 2 + core
    swap = lax.rem(core + x_hi, 2)
    target = m + swap * (3 - 2 * r)

    loads = [
        pltpu.make_async_copy(forcing, slab, load_sem.at[0]),
        pltpu.make_async_copy(table_in, table, load_sem.at[1]),
    ]
    window = pl.ds(pl.multiple_of(lax.div(target, 2) * 8, 8), 8)
    param_loads = [
        pltpu.make_async_copy(coupling.at[:, window], params.at[0], load_sem.at[2]),
        pltpu.make_async_copy(velocity.at[:, :, window], params.at[pl.ds(1, 3)], load_sem.at[3]),
        pltpu.make_async_copy(initial.at[:, window], params.at[4], load_sem.at[4]),
    ]
    for load in loads + param_loads:
        load.start()

    zeros = jnp.zeros((8, 128), F32)
    for g in range(GROUPS):
        for parity in range(2):
            for z in range(8):
                for y in range(8):
                    away = max(2 - z, z - 5, 0) + max(2 - y, y - 5, 0)
                    if 0 < away <= 2:
                        d[g, parity, z, y] = zeros
    near[...] = jnp.zeros_like(near)

    barrier = pltpu.get_barrier_semaphore()

    def greet(i, carry):
        t = lax.rem(me_t + 8 + i, 32)

        @pl.when(jnp.logical_or(t != me_t, swap == 1))
        def _():
            pl.semaphore_signal(barrier, inc=1, device_id=(t, row * 2 + core), device_id_type=MESH)

        return carry

    sides = [(-1, 0), (1, 0), (0, -1), (0, 1), (-1, -1), (1, 1), (-1, 1), (1, -1)]
    opposite = [1, 0, 3, 2, 5, 4, 7, 6]
    in_y = {-1: m > 0, 1: m < 31}
    in_z = {-1: zz > 0, 1: zz < 7}
    side_device, has = [], []
    for by, bz in sides:
        side_device.append(device_at(m + by, zz + bz))
        inside = in_y[by] if by else in_z[bz]
        has.append(jnp.logical_and(in_y[by], in_z[bz]) if by and bz else inside)
    count = 31 + swap
    for side in range(8):

        @pl.when(has[side])
        def _():
            pl.semaphore_signal(barrier, inc=1, device_id=side_device[side], device_id_type=MESH)

        count += has[side].astype(jnp.int32)
    lax.fori_loop(0, 32, greet, 0)

    low = lax.broadcasted_iota(jnp.int32, (8, 128), 0) < 4
    loads[0].wait()

    def pack(t, carry):
        rows = pl.ds(pl.multiple_of(t * 8, 8), 8)
        v = [slab[z, rows] for z in range(4)]
        w = [pltpu.roll(a, 4, 0) for a in v]
        packed[2 * t, 0:8] = jnp.where(low, v[0], w[1])
        packed[2 * t, 8:16] = jnp.where(low, v[2], w[3])
        packed[2 * t + 1, 0:8] = jnp.where(low, w[0], v[1])
        packed[2 * t + 1, 8:16] = jnp.where(low, w[2], v[3])
        return carry

    lax.fori_loop(0, 16, pack, 0)
    pl.semaphore_wait(barrier, count)

    def out_copy(i):
        return pltpu.make_async_remote_copy(
            src_ref=packed.at[i],
            dst_ref=times.at[me_t],
            send_sem=out_send.at[i],
            recv_sem=out_recv.at[me_t],
            device_id=device_at(i, row * 2 + x_hi),
            device_id_type=MESH,
        )

    def is_self(i):
        return jnp.logical_and(i == m, swap == 0)

    def out_start(k, carry):
        i = lax.rem(m + 1 + k, 32)

        @pl.when(jnp.logical_not(is_self(i)))
        def _():
            out_copy(i).start()

        return carry

    lax.fori_loop(0, 32, out_start, 0)

    @pl.when(swap == 0)
    def _():
        times[me_t] = packed[m]

    for load in param_loads:
        load.wait()
    odd = lax.rem(target, 2) == 1
    for f in range(5):
        v = [params[f, z] for z in range(4)]
        w = [pltpu.roll(a, 4, 0) for a in v]
        v, w = [jnp.where(odd, b, a) for a, b in zip(v, w)], [jnp.where(odd, a, b) for a, b in zip(v, w)]
        pack_params[f, 0:8] = jnp.where(low, v[0], w[1])
        pack_params[f, 8:16] = jnp.where(low, v[2], w[3])
    param_copy = pltpu.make_async_remote_copy(
        src_ref=pack_params,
        dst_ref=own_params,
        send_sem=param_send,
        recv_sem=param_recv,
        device_id=device_at(target, row * 2 + 1 - core),
        device_id_type=MESH,
    )
    @pl.when(swap == 1)
    def _():
        param_copy.start()
        param_copy.wait()

    @pl.when(swap == 0)
    def _():
        own_params[...] = pack_params[...]

    def near_copy(side):
        return pltpu.make_async_remote_copy(
            src_ref=own_params,
            dst_ref=near.at[side],
            send_sem=near_send.at[side],
            recv_sem=near_recv.at[side],
            device_id=side_device[side],
            device_id_type=MESH,
        )

    for side in range(4):

        @pl.when(has[side])
        def _():
            near_copy(side).start()

    lane = lax.broadcasted_iota(jnp.int32, (16, 128), 1)
    sub = lax.broadcasted_iota(jnp.int32, (16, 128), 0)
    loads[1].wait()

    def coefficients(ref):
        c = ref[0]
        flow = [c * ref[1 + k] for k in range(3)]
        return c, [
            c - flow[0],
            c + flow[0],
            c - flow[1],
            c + flow[1],
            jnp.where(lane == 127, 0.0, c - flow[2]),
            jnp.where(lane == 0, 0.0, c + flow[2]),
        ]

    def spread_coefficients(c, coefs, cells):
        middle = 1.0 + 6.0 * c
        for p, at in cells:
            for k in range(6):
                coef[at, k] = jnp.broadcast_to(coefs[k][p : p + 1], (8, 128))
            mid = jnp.broadcast_to(middle[p : p + 1], (8, 128))
            for g in range(GROUPS):
                d_re, d_im = mid - table[g, 0], table[g, 1]
                inv = 1.0 / (d_re * d_re + d_im * d_im)
                diag[g, at, 0] = d_re * inv
                diag[g, at, 1] = d_im * inv

    c, coefs = coefficients(own_params)
    spread_coefficients(c, coefs, [(p, p) for p in range(16)])
    for side in range(4):

        @pl.when(has[side])
        def _():
            near_copy(side).wait_send()

        @pl.when(has[opposite[side]])
        def _():
            near_copy(side).wait_recv()

    ring_rows = [[4 * i for i in range(4)], [4 * i + 3 for i in range(4)], range(4), range(12, 16)]
    for side in range(4):
        cells = [(p, 16 + side * 4 + i) for i, p in enumerate(ring_rows[side])]
        spread_coefficients(*coefficients(near.at[side]), cells)
    own = own_params[4]
    after_y, before_y, after_z, before_z = [near[side, 4] for side in range(4)]
    step = lax.rem(sub, 4)
    summed = coefs[0] * jnp.where(sub < 12, pltpu.roll(own, 12, 0), pltpu.roll(after_z, 12, 0))
    summed += coefs[1] * jnp.where(sub >= 4, pltpu.roll(own, 4, 0), pltpu.roll(before_z, 4, 0))
    summed += coefs[2] * jnp.where(step < 3, pltpu.roll(own, 15, 0), pltpu.roll(after_y, 3, 0))
    summed += coefs[3] * jnp.where(step > 0, pltpu.roll(own, 1, 0), pltpu.roll(before_y, 13, 0))
    summed += coefs[4] * pltpu.roll(own, 127, 1) + coefs[5] * pltpu.roll(own, 1, 1)
    source = summed - 6.0 * c * own

    def out_finish(i, carry):
        @pl.when(jnp.logical_not(is_self(i)))
        def _():
            out_copy(i).wait_send()

        @pl.when(jnp.logical_or(i != me_t, swap == 1))
        def _():
            pltpu.make_async_remote_copy(
                src_ref=packed.at[i],
                dst_ref=times.at[i],
                send_sem=out_send.at[i],
                recv_sem=out_recv.at[i],
                device_id=(me_t, me_s),
                device_id_type=MESH,
            ).wait_recv()

        return carry

    lax.fori_loop(0, 32, out_finish, 0)

    def transform(h, carry):
        rows = pl.ds(pl.multiple_of(h * 8, 8), 8)
        re, im = real_fft([GAMMA[n] * times[n, rows] for n in range(32)])
        for j in range(17):
            spread[pl.ds(h * 256 + unit_of(j, False), 8, stride=32), :] = re[j]
            if im[j] is not None:
                spread[pl.ds(h * 256 + unit_of(j, True), 8, stride=32), :] = im[j]
        return carry

    lax.fori_loop(0, 2, transform, 0)

    def halo_copy(g, parity, side):
        refs = []
        for shift in (0, 4):
            at = []
            for by, bz in ((sides[side][1], sides[side][0]), (sides[side][0], sides[side][1])):
                if by == 0:
                    at.append(pl.ds(2, 4))
                elif bz == 0:
                    at.append(pl.ds((2 if by < 0 else 4) - by * shift, 2))
                else:
                    at.append((2 if by < 0 else 5) - by * shift)
            refs.append(d.at[g, parity, at[0], at[1]])
        return pltpu.make_async_remote_copy(
            src_ref=refs[0],
            dst_ref=refs[1],
            send_sem=halo_send.at[g, parity, side],
            recv_sem=halo_recv.at[g, parity, side],
            device_id=side_device[side],
            device_id_type=MESH,
        )

    def halo_start(g, parity):
        for side in range(8):

            @pl.when(has[side])
            def _():
                halo_copy(g, parity, side).start()

    def halo_wait(g, parity):
        for side in range(8):

            @pl.when(has[side])
            def _():
                halo_copy(g, parity, side).wait_send()
                halo_copy(g, parity, opposite[side]).wait_recv()

    def divide(g, at, s):
        return diag[g, at, 0] * s + diag[g, at, 1] * pltpu.roll(s, 4, 0)

    def stencil(field, z, y, at):
        here = field[z, y]
        s = coef[at, 0] * field[z + 1, y]
        s += coef[at, 1] * field[z - 1, y]
        s += coef[at, 2] * field[z, y + 1]
        s += coef[at, 3] * field[z, y - 1]
        s += coef[at, 4] * pltpu.roll(here, 127, 1)
        s += coef[at, 5] * pltpu.roll(here, 1, 1)
        return s

    for g in range(GROUPS):
        for p in range(16):
            z, y = p // 4, p % 4
            base = jnp.broadcast_to(source[p : p + 1], (8, 128))
            rows = pl.ds(p * 32 + g * 8, 8)
            v = divide(g, p, spread[rows] + table[g, 2] * base)
            d[g, 0, z + 2, y + 2] = v
            total[rows] = v
        halo_start(g, 0)

    ring = [(i, -1) for i in range(4)] + [(i, 4) for i in range(4)]
    ring = ring + [(-1, i) for i in range(4)] + [(4, i) for i in range(4)]
    ring = ring[4:8] + ring[0:4] + ring[12:16] + ring[8:12]

    def two_sweeps(g, parity, send):
        halo_wait(g, parity)
        old, new = d.at[g, parity], d.at[g, 1 - parity]
        for at in range(32):
            z, y = (at // 4, at % 4) if at < 16 else ring[at - 16]
            v = divide(g, at, stencil(old, z + 2, y + 2, at))
            middle_d[z + 1, y + 1] = v
            if at < 16:
                total[pl.ds(at * 32 + g * 8, 8)] += v
        for at in range(16):
            z, y = at // 4, at % 4
            v = divide(g, at, stencil(middle_d, z + 1, y + 1, at))
            new[z + 2, y + 2] = v
            total[pl.ds(at * 32 + g * 8, 8)] += v
        if send:
            halo_start(g, 1 - parity)

    def all_groups(k, carry):
        for g in range(GROUPS):
            two_sweeps(g, lax.rem(k, 2), True)
        return carry

    lax.fori_loop(0, 4, all_groups, 0)
    for p in range(16):
        s = jnp.zeros((8, 128), F32)
        for g in range(GROUPS):
            s += table[g, 3] * total[pl.ds(p * 32 + g * 8, 8)]
        wrap[p] = jnp.broadcast_to(jnp.sum(s, axis=0, keepdims=True), (8, 128))
    for g in range(GROUPS):
        halo_wait(g, 0)
        for at in range(16):
            z, y = at // 4, at % 4
            s = stencil(d.at[g, 0], z + 2, y + 2, at) - table[g, 4] * wrap[at]
            v = divide(g, at, s)
            d[g, 1, z + 2, y + 2] = v
            total[pl.ds(at * 32 + g * 8, 8)] += v
        halo_start(g, 1)
    lax.fori_loop(5, 8, all_groups, 0)
    for g in range(GROUPS):
        two_sweeps(g, 0, False)

    def restore(h, carry):
        rows = pl.ds(pl.multiple_of(h * 8, 8), 8)
        re, im = [None] * 17, [None] * 17
        for j in range(17):
            re[j] = total[pl.ds(h * 256 + unit_of(j, False), 8, stride=32), :]
            if 0 < j < 16:
                im[j] = total[pl.ds(h * 256 + unit_of(j, True), 8, stride=32), :]
        for n, value in enumerate(real_ifft(re, im)):
            back[n, rows] = value * (1.0 / (STEPS * GAMMA[n]))
        return carry

    lax.fori_loop(0, 2, restore, 0)

    def back_copy(i):
        return pltpu.make_async_remote_copy(
            src_ref=back.at[i],
            dst_ref=gathered.at[m],
            send_sem=back_send.at[i],
            recv_sem=back_recv.at[m],
            device_id=(i, row * 2 + core),
            device_id_type=MESH,
        )

    def is_own(i):
        return jnp.logical_and(i == me_t, swap == 0)

    def back_start(k, carry):
        i = lax.rem(me_t + 1 + k, 32)

        @pl.when(jnp.logical_not(is_own(i)))
        def _():
            back_copy(i).start()

        return carry

    lax.fori_loop(0, 32, back_start, 0)

    @pl.when(swap == 0)
    def _():
        gathered[m] = back[me_t]

    def back_finish(i, carry):
        @pl.when(jnp.logical_not(is_own(i)))
        def _():
            back_copy(i).wait_send()

        @pl.when(jnp.logical_not(is_self(i)))
        def _():
            pltpu.make_async_remote_copy(
                src_ref=back.at[i],
                dst_ref=gathered.at[i],
                send_sem=back_send.at[i],
                recv_sem=back_recv.at[i],
                device_id=(me_t, me_s),
                device_id_type=MESH,
            ).wait_recv()

        return carry

    lax.fori_loop(0, 32, back_finish, 0)

    def unpack(t, carry):
        rows = pl.ds(pl.multiple_of(t * 8, 8), 8)
        p = [gathered[2 * t, 0:8], gathered[2 * t, 8:16]]
        q = [gathered[2 * t + 1, 0:8], gathered[2 * t + 1, 8:16]]
        for i in range(2):
            out[2 * i, rows] = jnp.where(low, p[i], pltpu.roll(q[i], 4, 0))
            out[2 * i + 1, rows] = jnp.where(low, pltpu.roll(p[i], 4, 0), q[i])
        return carry

    lax.fori_loop(0, 16, unpack, 0)


def body(forcing, initial, coupling, velocity):
    local = forcing.shape[1:]
    table = jnp.asarray(unit_tables())
    hbm = pl.BlockSpec(memory_space=pl.ANY)
    dma = pltpu.SemaphoreType.DMA
    correction = pl.pallas_call(
        kernel,
        out_shape=jax.ShapeDtypeStruct(local, F32),
        in_specs=[hbm] * 5,
        out_specs=pl.BlockSpec(memory_space=pltpu.VMEM),
        scratch_shapes=[
            pltpu.VMEM(local, F32),
            pltpu.VMEM((5, 4, 8, 128), F32),
            pltpu.VMEM((GROUPS, 5, 8, 128), F32),
            pltpu.VMEM((32, 16, 128), F32),
            pltpu.VMEM((32, 16, 128), F32),
            pltpu.VMEM((512, 128), F32),
            pltpu.VMEM((32, 16, 128), F32),
            pltpu.VMEM((32, 16, 128), F32),
            pltpu.VMEM((5, 16, 128), F32),
            pltpu.VMEM((5, 16, 128), F32),
            pltpu.VMEM((4, 5, 16, 128), F32),
            pltpu.VMEM((32, 6, 8, 128), F32),
            pltpu.VMEM((GROUPS, 32, 2, 8, 128), F32),
            pltpu.VMEM((GROUPS, 2, 8, 8, 8, 128), F32),
            pltpu.VMEM((6, 6, 8, 128), F32),
            pltpu.VMEM((512, 128), F32),
            pltpu.VMEM((16, 8, 128), F32),
            dma((5,)),
            dma((32,)),
            dma((32,)),
            dma((32,)),
            dma((32,)),
            dma,
            dma,
            dma((4,)),
            dma((4,)),
            dma((GROUPS, 2, 8)),
            dma((GROUPS, 2, 8)),
        ],
        compiler_params=pltpu.CompilerParams(collective_id=0, has_side_effects=True),
    )(forcing[0], initial, coupling, velocity, table)
    return (initial + correction)[None]


def solution(mesh):
    return jax.shard_map(
        body,
        mesh=mesh,
        in_specs=(
            P("tm", "space", None, None),
            P("space", None, None),
            P("space", None, None),
            P(None, "space", None, None),
        ),
        out_specs=P("tm", "space", None, None),
        check_vma=False,
    )
```

```python
import functools
import math

import jax
import jax.numpy as jnp
import numpy as np
from jax import lax
from jax.experimental import pallas as pl
from jax.experimental.pallas import tpu as pltpu
from jax.sharding import PartitionSpec as P

STEPS = 32
ALPHA = 0.1
RHO = ALPHA ** (1.0 / STEPS)
GAMMA = [ALPHA ** (n / STEPS) for n in range(STEPS)]
GROUPS = 4
SLOTS = STEPS // 2 // GROUPS
MESH = pl.DeviceIdType.MESH
F32 = jnp.float32


def real_fft(xs):
    size = len(xs)
    if size == 2:
        return [xs[0] + xs[1], xs[0] - xs[1]], [None, None]
    even_re, even_im = real_fft(xs[0::2])
    odd_re, odd_im = real_fft(xs[1::2])
    half, quarter = size // 2, size // 4
    re, im = [None] * (half + 1), [None] * (half + 1)
    re[0], re[half] = even_re[0] + odd_re[0], even_re[0] - odd_re[0]
    for j in range(1, quarter):
        c, s = math.cos(2 * math.pi * j / size), math.sin(2 * math.pi * j / size)
        t_re = c * odd_re[j] + s * odd_im[j]
        t_im = c * odd_im[j] - s * odd_re[j]
        re[j], im[j] = even_re[j] + t_re, even_im[j] + t_im
        re[half - j], im[half - j] = even_re[j] - t_re, t_im - even_im[j]
    re[quarter], im[quarter] = even_re[quarter], -odd_re[quarter]
    return re, im


def real_ifft(re, im):
    half = len(re) - 1
    size = 2 * half
    if size == 2:
        return [re[0] + re[1], re[0] - re[1]]
    quarter = size // 4
    even_re, even_im = [None] * (quarter + 1), [None] * (quarter + 1)
    odd_re, odd_im = [None] * (quarter + 1), [None] * (quarter + 1)
    even_re[0], odd_re[0] = re[0] + re[half], re[0] - re[half]
    for j in range(1, quarter):
        c, s = math.cos(2 * math.pi * j / size), math.sin(2 * math.pi * j / size)
        even_re[j], even_im[j] = re[j] + re[half - j], im[j] - im[half - j]
        t_re, t_im = re[j] - re[half - j], im[j] + im[half - j]
        odd_re[j], odd_im[j] = c * t_re - s * t_im, c * t_im + s * t_re
    even_re[quarter], odd_re[quarter] = 2.0 * re[quarter], -2.0 * im[quarter]
    even = real_ifft(even_re, even_im)
    odd = real_ifft(odd_re, odd_im)
    return [(even, odd)[n % 2][n // 2] for n in range(size)]


def unit_tables():
    slots = STEPS // 2
    j = np.arange(slots)
    theta = 2 * np.pi * j / STEPS
    n = np.arange(STEPS)
    gamma = np.array(GAMMA)
    angle = 2 * np.pi * ((j[:, None] * n[None, :]) % STEPS) / STEPS
    last = 2 * np.pi * ((j * (STEPS - 1)) % STEPS) / STEPS
    re = np.stack(
        [
            RHO * np.cos(theta),
            RHO * np.sin(theta),
            (np.cos(angle) * gamma).sum(1),
            2 * np.cos(last) * RHO / STEPS,
            np.ones(slots),
        ]
    )
    im = np.stack(
        [
            RHO * np.cos(theta),
            -RHO * np.sin(theta),
            -(np.sin(angle) * gamma).sum(1),
            -2 * np.sin(last) * RHO / STEPS,
            np.zeros(slots),
        ]
    )
    re[1, 0] = im[1, 0] = 0.0
    re[3, 0] = RHO / STEPS
    im[:, 0] = [-RHO, 0.0, (gamma * (-1.0) ** n).sum(), -RHO / STEPS, 1.0]
    rows = np.concatenate([re.reshape(5, GROUPS, SLOTS), im.reshape(5, GROUPS, SLOTS)], axis=2)
    rows = rows.transpose(1, 0, 2)[..., None]
    return np.ascontiguousarray(np.broadcast_to(rows, (GROUPS, 5, 8, 128))).astype(np.float32)


def unit_of(j, imaginary):
    if j == STEPS // 2:
        j, imaginary = 0, True
    return (j // SLOTS) * 8 + (SLOTS if imaginary else 0) + j % SLOTS


def device_at(m, zz):
    r, along = lax.rem(m, 4), lax.div(m, 4)
    x = r + lax.rem(along, 2) * (3 - 2 * r)
    return (
        lax.rem(x, 2) * 16 + along * 2 + lax.rem(zz, 2),
        lax.div(zz, 2) * 2 + lax.div(x, 2),
    )


def kernel(
    forcing,
    initial,
    coupling,
    velocity,
    table_in,
    out,
    slab,
    params,
    table,
    packed,
    times,
    spread,
    back,
    gathered,
    pack_params,
    own_params,
    near,
    coef,
    diag,
    d,
    middle_d,
    total,
    wrap,
    load_sem,
    out_send,
    out_recv,
    back_send,
    back_recv,
    param_send,
    param_recv,
    near_send,
    near_recv,
    halo_send,
    halo_recv,
):
    me_t, me_s = lax.axis_index("tm"), lax.axis_index("space")
    core, along = lax.rem(me_t, 2), lax.rem(lax.div(me_t, 2), 8)
    row, x_hi = lax.div(me_s, 2), lax.rem(me_s, 2)
    x = 2 * x_hi + lax.div(me_t, 16)
    r = x + lax.rem(along, 2) * (3 - 2 * x)
    m = along * 4 + r
    zz = row * 2 + core
    swap = lax.rem(core + x_hi, 2)
    target = m + swap * (3 - 2 * r)
    x_lo = x - 2 * x_hi

    far_first = (4, 3, 5, 2, 6, 1, 7, 0)
    zs, turned = [None] * 8, [None] * 8
    odd_z = lax.rem(along, 2)
    for step in range(8):
        zs[step] = along + step - 8 * (along + step >= 8).astype(jnp.int32)
        turned[step] = 1 - odd_z if step % 2 else odd_z
    xs = [x + step - 4 * (x + step >= 4).astype(jnp.int32) for step in range(4)]
    x_his = [(v >= 2).astype(jnp.int32) for v in xs]

    loads = [
        pltpu.make_async_copy(forcing, slab, load_sem.at[0]),
        pltpu.make_async_copy(table_in, table, load_sem.at[1]),
    ]
    window = pl.ds(pl.multiple_of(lax.div(target, 2) * 8, 8), 8)
    param_loads = [
        pltpu.make_async_copy(coupling.at[:, window], params.at[0], load_sem.at[2]),
        pltpu.make_async_copy(velocity.at[:, :, window], params.at[pl.ds(1, 3)], load_sem.at[3]),
        pltpu.make_async_copy(initial.at[:, window], params.at[4], load_sem.at[4]),
    ]
    for load in loads + param_loads:
        load.start()

    barrier = pltpu.get_barrier_semaphore()

    sides = [(-1, 0), (1, 0), (0, -1), (0, 1), (-1, -1), (1, 1), (-1, 1), (1, -1)]
    opposite = [1, 0, 3, 2, 5, 4, 7, 6]
    in_y = {-1: m > 0, 1: m < 31}
    in_z = {-1: zz > 0, 1: zz < 7}
    side_device, has = [], []
    for by, bz in sides:
        side_device.append(device_at(m + by, zz + bz))
        inside = in_y[by] if by else in_z[bz]
        has.append(jnp.logical_and(in_y[by], in_z[bz]) if by and bz else inside)
    interior = jnp.logical_and(jnp.logical_and(has[0], has[1]), jnp.logical_and(has[2], has[3]))

    @pl.when(jnp.logical_not(interior))
    def _():
        zeros = jnp.zeros((8, 128), F32)
        for g in range(GROUPS):
            for parity in range(2):
                for z in range(8):
                    for y in range(8):
                        away = max(2 - z, z - 5, 0) + max(2 - y, y - 5, 0)
                        if 0 < away <= 2:
                            d[g, parity, z, y] = zeros
        near[...] = jnp.zeros_like(near)

    count = 31 + swap
    def senders():
        for step in far_first:
            for flip_x in range(2):
                for flip_core in range(2):
                    to_x = 1 - x_lo if flip_x else x_lo
                    to_core = 1 - core if flip_core else core
                    t = to_x * 16 + zs[step] * 2 + to_core
                    yield t, step == 0 and flip_x == 0 and flip_core == 0

    for t, mine in senders():

        @pl.when(swap == 1 if mine else True)
        def _():
            pl.semaphore_signal(barrier, inc=1, device_id=(t, row * 2 + core), device_id_type=MESH)

    for side in range(8):

        @pl.when(has[side])
        def _():
            pl.semaphore_signal(barrier, inc=1, device_id=side_device[side], device_id_type=MESH)

        count += has[side].astype(jnp.int32)

    low = lax.broadcasted_iota(jnp.int32, (8, 128), 0) < 4
    loads[0].wait()

    def pack(t, carry):
        rows = pl.ds(pl.multiple_of(t * 8, 8), 8)
        v = [slab[z, rows] for z in range(4)]
        w = [pltpu.roll(a, 4, 0) for a in v]
        packed[2 * t, 0:8] = jnp.where(low, v[0], w[1])
        packed[2 * t, 8:16] = jnp.where(low, v[2], w[3])
        packed[2 * t + 1, 0:8] = jnp.where(low, w[0], v[1])
        packed[2 * t + 1, 8:16] = jnp.where(low, w[2], v[3])
        return carry

    lax.fori_loop(0, 16, pack, 0)
    pl.semaphore_wait(barrier, count)

    for step in far_first:
        for to_x in range(4):
            chunk = 4 * zs[step] + xs[to_x] + turned[step] * (3 - 2 * xs[to_x])
            to = (
                (xs[to_x] - 2 * x_his[to_x]) * 16 + zs[step] * 2 + x_hi,
                row * 2 + x_his[to_x],
            )

            @pl.when(swap == 1 if step == 0 and to_x == 0 else True)
            def _():
                pltpu.make_async_remote_copy(
                    src_ref=packed.at[chunk],
                    dst_ref=times.at[me_t],
                    send_sem=out_send,
                    recv_sem=out_recv,
                    device_id=to,
                    device_id_type=MESH,
                ).start()

    @pl.when(swap == 0)
    def _():
        times[me_t] = packed[m]

    def finish(src, dst, send_sem, recv_sem):
        for copies in range(2):

            @pl.when(swap == copies)
            def _():
                some = pl.ds(0, 31 + copies)
                pltpu.make_async_remote_copy(
                    src_ref=src.at[some],
                    dst_ref=dst.at[some],
                    send_sem=send_sem,
                    recv_sem=recv_sem,
                    device_id=(me_t, me_s),
                    device_id_type=MESH,
                ).wait()

    for load in param_loads:
        load.wait()
    odd = lax.rem(target, 2) == 1
    for f in range(5):
        v = [params[f, z] for z in range(4)]
        w = [pltpu.roll(a, 4, 0) for a in v]
        v, w = [jnp.where(odd, b, a) for a, b in zip(v, w)], [jnp.where(odd, a, b) for a, b in zip(v, w)]
        pack_params[f, 0:8] = jnp.where(low, v[0], w[1])
        pack_params[f, 8:16] = jnp.where(low, v[2], w[3])
    param_copy = pltpu.make_async_remote_copy(
        src_ref=pack_params,
        dst_ref=own_params,
        send_sem=param_send,
        recv_sem=param_recv,
        device_id=device_at(target, row * 2 + 1 - core),
        device_id_type=MESH,
    )
    @pl.when(swap == 1)
    def _():
        param_copy.start()
        param_copy.wait()

    @pl.when(swap == 0)
    def _():
        own_params[...] = pack_params[...]

    def near_copy(side):
        return pltpu.make_async_remote_copy(
            src_ref=own_params,
            dst_ref=near.at[side],
            send_sem=near_send.at[side],
            recv_sem=near_recv.at[side],
            device_id=side_device[side],
            device_id_type=MESH,
        )

    for side in range(4):

        @pl.when(has[side])
        def _():
            near_copy(side).start()

    lane = lax.broadcasted_iota(jnp.int32, (16, 128), 1)
    sub = lax.broadcasted_iota(jnp.int32, (16, 128), 0)
    loads[1].wait()

    def coefficients(ref):
        c = ref[0]
        flow = [c * ref[1 + k] for k in range(3)]
        return c, [
            c - flow[0],
            c + flow[0],
            c - flow[1],
            c + flow[1],
            jnp.where(lane == 127, 0.0, c - flow[2]),
            jnp.where(lane == 0, 0.0, c + flow[2]),
        ]

    def spread_coefficients(c, coefs, cells):
        middle = 1.0 + 6.0 * c
        for p, at in cells:
            for k in range(6):
                coef[at, k] = jnp.broadcast_to(coefs[k][p : p + 1], (8, 128))
            mid = jnp.broadcast_to(middle[p : p + 1], (8, 128))
            for g in range(GROUPS):
                d_re, d_im = mid - table[g, 0], table[g, 1]
                inv = 1.0 / (d_re * d_re + d_im * d_im)
                diag[g, at, 0] = d_re * inv
                diag[g, at, 1] = d_im * inv

    c, coefs = coefficients(own_params)
    spread_coefficients(c, coefs, [(p, p) for p in range(16)])
    for side in range(4):

        @pl.when(has[side])
        def _():
            near_copy(side).wait_send()

        @pl.when(has[opposite[side]])
        def _():
            near_copy(side).wait_recv()

    ring_rows = [[4 * i for i in range(4)], [4 * i + 3 for i in range(4)], range(4), range(12, 16)]
    for side in range(4):
        cells = [(p, 16 + side * 4 + i) for i, p in enumerate(ring_rows[side])]
        spread_coefficients(*coefficients(near.at[side]), cells)
    own = own_params[4]
    after_y, before_y, after_z, before_z = [near[side, 4] for side in range(4)]
    step = lax.rem(sub, 4)
    summed = coefs[0] * jnp.where(sub < 12, pltpu.roll(own, 12, 0), pltpu.roll(after_z, 12, 0))
    summed += coefs[1] * jnp.where(sub >= 4, pltpu.roll(own, 4, 0), pltpu.roll(before_z, 4, 0))
    summed += coefs[2] * jnp.where(step < 3, pltpu.roll(own, 15, 0), pltpu.roll(after_y, 3, 0))
    summed += coefs[3] * jnp.where(step > 0, pltpu.roll(own, 1, 0), pltpu.roll(before_y, 13, 0))
    summed += coefs[4] * pltpu.roll(own, 127, 1) + coefs[5] * pltpu.roll(own, 1, 1)
    source = summed - 6.0 * c * own

    finish(packed, times, out_send, out_recv)

    def transform(h, carry):
        rows = pl.ds(pl.multiple_of(h * 8, 8), 8)
        re, im = real_fft([GAMMA[n] * times[n, rows] for n in range(32)])
        for j in range(17):
            spread[pl.ds(h * 256 + unit_of(j, False), 8, stride=32), :] = re[j]
            if im[j] is not None:
                spread[pl.ds(h * 256 + unit_of(j, True), 8, stride=32), :] = im[j]
        return carry

    lax.fori_loop(0, 2, transform, 0)

    def halo_copy(g, parity, side):
        refs = []
        for shift in (0, 4):
            at = []
            for by, bz in ((sides[side][1], sides[side][0]), (sides[side][0], sides[side][1])):
                if by == 0:
                    at.append(pl.ds(2, 4))
                elif bz == 0:
                    at.append(pl.ds((2 if by < 0 else 4) - by * shift, 2))
                else:
                    at.append((2 if by < 0 else 5) - by * shift)
            refs.append(d.at[g, parity, at[0], at[1]])
        return pltpu.make_async_remote_copy(
            src_ref=refs[0],
            dst_ref=refs[1],
            send_sem=halo_send.at[g, parity],
            recv_sem=halo_recv.at[g, parity],
            device_id=side_device[side],
            device_id_type=MESH,
        )

    def halo_start(g, parity):
        @pl.when(interior)
        def _():
            for side in range(8):
                halo_copy(g, parity, side).start()

        @pl.when(jnp.logical_not(interior))
        def _():
            for side in range(8):

                @pl.when(has[side])
                def _():
                    halo_copy(g, parity, side).start()

    whole_y, whole_z = jnp.logical_and(has[0], has[1]), jnp.logical_and(has[2], has[3])

    def halo_wait(g, parity):
        for tiles, when in (
            (36, interior),
            (26, whole_y != whole_z),
            (17, jnp.logical_not(jnp.logical_or(whole_y, whole_z))),
        ):

            @pl.when(when)
            def _():
                amount = spread.at[pl.ds(0, tiles * 8)]
                pltpu.make_async_remote_copy(
                    src_ref=amount,
                    dst_ref=amount,
                    send_sem=halo_send.at[g, parity],
                    recv_sem=halo_recv.at[g, parity],
                    device_id=(me_t, me_s),
                    device_id_type=MESH,
                ).wait()

    def divide(g, at, s):
        return diag[g, at, 0] * s + diag[g, at, 1] * pltpu.roll(s, 4, 0)

    def stencil(field, z, y, at):
        here = field[z, y]
        s = coef[at, 0] * field[z + 1, y]
        s += coef[at, 1] * field[z - 1, y]
        s += coef[at, 2] * field[z, y + 1]
        s += coef[at, 3] * field[z, y - 1]
        s += coef[at, 4] * pltpu.roll(here, 127, 1)
        s += coef[at, 5] * pltpu.roll(here, 1, 1)
        return s

    for g in range(GROUPS):
        for p in range(16):
            z, y = p // 4, p % 4
            base = jnp.broadcast_to(source[p : p + 1], (8, 128))
            rows = pl.ds(p * 32 + g * 8, 8)
            v = divide(g, p, spread[rows] + table[g, 2] * base)
            d[g, 0, z + 2, y + 2] = v
            total[rows] = v
        halo_start(g, 0)

    ring = [(i, -1) for i in range(4)] + [(i, 4) for i in range(4)]
    ring = ring + [(-1, i) for i in range(4)] + [(4, i) for i in range(4)]
    ring = ring[4:8] + ring[0:4] + ring[12:16] + ring[8:12]

    def two_sweeps(g, parity, send):
        halo_wait(g, parity)
        old, new = d.at[g, parity], d.at[g, 1 - parity]
        for at in range(32):
            z, y = (at // 4, at % 4) if at < 16 else ring[at - 16]
            v = divide(g, at, stencil(old, z + 2, y + 2, at))
            middle_d[z + 1, y + 1] = v
            if at < 16:
                total[pl.ds(at * 32 + g * 8, 8)] += v
        for at in range(16):
            z, y = at // 4, at % 4
            v = divide(g, at, stencil(middle_d, z + 1, y + 1, at))
            new[z + 2, y + 2] = v
            total[pl.ds(at * 32 + g * 8, 8)] += v
        if send:
            halo_start(g, 1 - parity)

    def all_groups(k, carry):
        for g in range(GROUPS):
            two_sweeps(g, lax.rem(k, 2), True)
        return carry

    lax.fori_loop(0, 4, all_groups, 0)
    for p in range(16):
        s = jnp.zeros((8, 128), F32)
        for g in range(GROUPS):
            s += table[g, 3] * total[pl.ds(p * 32 + g * 8, 8)]
        wrap[p] = jnp.broadcast_to(jnp.sum(s, axis=0, keepdims=True), (8, 128))
    for g in range(GROUPS):
        halo_wait(g, 0)
        for at in range(16):
            z, y = at // 4, at % 4
            s = stencil(d.at[g, 0], z + 2, y + 2, at) - table[g, 4] * wrap[at]
            v = divide(g, at, s)
            d[g, 1, z + 2, y + 2] = v
            total[pl.ds(at * 32 + g * 8, 8)] += v
        halo_start(g, 1)
    lax.fori_loop(5, 8, all_groups, 0)
    for g in range(GROUPS):
        two_sweeps(g, 0, False)

    def restore(h, carry):
        rows = pl.ds(pl.multiple_of(h * 8, 8), 8)
        re, im = [None] * 17, [None] * 17
        for j in range(17):
            re[j] = total[pl.ds(h * 256 + unit_of(j, False), 8, stride=32), :]
            if 0 < j < 16:
                im[j] = total[pl.ds(h * 256 + unit_of(j, True), 8, stride=32), :]
        for n, value in enumerate(real_ifft(re, im)):
            back[n, rows] = value * (1.0 / (STEPS * GAMMA[n]))
        return carry

    lax.fori_loop(0, 2, restore, 0)

    for t, mine in senders():

        @pl.when(swap == 1 if mine else True)
        def _():
            pltpu.make_async_remote_copy(
                src_ref=back.at[t],
                dst_ref=gathered.at[m],
                send_sem=back_send,
                recv_sem=back_recv,
                device_id=(t, row * 2 + core),
                device_id_type=MESH,
            ).start()

    @pl.when(swap == 0)
    def _():
        gathered[m] = back[me_t]

    finish(back, gathered, back_send, back_recv)

    def unpack(t, carry):
        rows = pl.ds(pl.multiple_of(t * 8, 8), 8)
        p = [gathered[2 * t, 0:8], gathered[2 * t, 8:16]]
        q = [gathered[2 * t + 1, 0:8], gathered[2 * t + 1, 8:16]]
        for i in range(2):
            out[2 * i, rows] = jnp.where(low, p[i], pltpu.roll(q[i], 4, 0))
            out[2 * i + 1, rows] = jnp.where(low, pltpu.roll(p[i], 4, 0), q[i])
        return carry

    lax.fori_loop(0, 16, unpack, 0)


def body(forcing, initial, coupling, velocity):
    local = forcing.shape[1:]
    table = jnp.asarray(unit_tables())
    hbm = pl.BlockSpec(memory_space=pl.ANY)
    dma = pltpu.SemaphoreType.DMA
    correction = pl.pallas_call(
        kernel,
        out_shape=jax.ShapeDtypeStruct(local, F32),
        in_specs=[hbm] * 5,
        out_specs=pl.BlockSpec(memory_space=pltpu.VMEM),
        scratch_shapes=[
            pltpu.VMEM(local, F32),
            pltpu.VMEM((5, 4, 8, 128), F32),
            pltpu.VMEM((GROUPS, 5, 8, 128), F32),
            pltpu.VMEM((32, 16, 128), F32),
            pltpu.VMEM((32, 16, 128), F32),
            pltpu.VMEM((512, 128), F32),
            pltpu.VMEM((32, 16, 128), F32),
            pltpu.VMEM((32, 16, 128), F32),
            pltpu.VMEM((5, 16, 128), F32),
            pltpu.VMEM((5, 16, 128), F32),
            pltpu.VMEM((4, 5, 16, 128), F32),
            pltpu.VMEM((32, 6, 8, 128), F32),
            pltpu.VMEM((GROUPS, 32, 2, 8, 128), F32),
            pltpu.VMEM((GROUPS, 2, 8, 8, 8, 128), F32),
            pltpu.VMEM((6, 6, 8, 128), F32),
            pltpu.VMEM((512, 128), F32),
            pltpu.VMEM((16, 8, 128), F32),
            dma((5,)),
            dma,
            dma,
            dma,
            dma,
            dma,
            dma,
            dma((4,)),
            dma((4,)),
            dma((GROUPS, 2)),
            dma((GROUPS, 2)),
        ],
        compiler_params=pltpu.CompilerParams(collective_id=0, has_side_effects=True),
    )(forcing[0], initial, coupling, velocity, table)
    return (initial + correction)[None]


def solution(mesh):
    return jax.shard_map(
        body,
        mesh=mesh,
        in_specs=(
            P("tm", "space", None, None),
            P("space", None, None),
            P("space", None, None),
            P(None, "space", None, None),
        ),
        out_specs=P("tm", "space", None, None),
        check_vma=False,
    )
```

```python
import functools
import math

import jax
import jax.numpy as jnp
import numpy as np
from jax import lax
from jax.experimental import pallas as pl
from jax.experimental.pallas import tpu as pltpu
from jax.sharding import PartitionSpec as P

STEPS = 32
ALPHA = 0.1
RHO = ALPHA ** (1.0 / STEPS)
GAMMA = [ALPHA ** (n / STEPS) for n in range(STEPS)]
GROUPS = 4
SLOTS = STEPS // 2 // GROUPS
MESH = pl.DeviceIdType.MESH
F32 = jnp.float32


def real_fft(xs):
    size = len(xs)
    if size == 2:
        return [xs[0] + xs[1], xs[0] - xs[1]], [None, None]
    even_re, even_im = real_fft(xs[0::2])
    odd_re, odd_im = real_fft(xs[1::2])
    half, quarter = size // 2, size // 4
    re, im = [None] * (half + 1), [None] * (half + 1)
    re[0], re[half] = even_re[0] + odd_re[0], even_re[0] - odd_re[0]
    for j in range(1, quarter):
        c, s = math.cos(2 * math.pi * j / size), math.sin(2 * math.pi * j / size)
        t_re = c * odd_re[j] + s * odd_im[j]
        t_im = c * odd_im[j] - s * odd_re[j]
        re[j], im[j] = even_re[j] + t_re, even_im[j] + t_im
        re[half - j], im[half - j] = even_re[j] - t_re, t_im - even_im[j]
    re[quarter], im[quarter] = even_re[quarter], -odd_re[quarter]
    return re, im


def real_ifft(re, im):
    half = len(re) - 1
    size = 2 * half
    if size == 2:
        return [re[0] + re[1], re[0] - re[1]]
    quarter = size // 4
    even_re, even_im = [None] * (quarter + 1), [None] * (quarter + 1)
    odd_re, odd_im = [None] * (quarter + 1), [None] * (quarter + 1)
    even_re[0], odd_re[0] = re[0] + re[half], re[0] - re[half]
    for j in range(1, quarter):
        c, s = math.cos(2 * math.pi * j / size), math.sin(2 * math.pi * j / size)
        even_re[j], even_im[j] = re[j] + re[half - j], im[j] - im[half - j]
        t_re, t_im = re[j] - re[half - j], im[j] + im[half - j]
        odd_re[j], odd_im[j] = c * t_re - s * t_im, c * t_im + s * t_re
    even_re[quarter], odd_re[quarter] = 2.0 * re[quarter], -2.0 * im[quarter]
    even = real_ifft(even_re, even_im)
    odd = real_ifft(odd_re, odd_im)
    return [(even, odd)[n % 2][n // 2] for n in range(size)]


def unit_tables():
    slots = STEPS // 2
    j = np.arange(slots)
    theta = 2 * np.pi * j / STEPS
    n = np.arange(STEPS)
    gamma = np.array(GAMMA)
    angle = 2 * np.pi * ((j[:, None] * n[None, :]) % STEPS) / STEPS
    last = 2 * np.pi * ((j * (STEPS - 1)) % STEPS) / STEPS
    re = np.stack(
        [
            RHO * np.cos(theta),
            RHO * np.sin(theta),
            (np.cos(angle) * gamma).sum(1),
            2 * np.cos(last) * RHO / STEPS,
            np.ones(slots),
        ]
    )
    im = np.stack(
        [
            RHO * np.cos(theta),
            -RHO * np.sin(theta),
            -(np.sin(angle) * gamma).sum(1),
            -2 * np.sin(last) * RHO / STEPS,
            np.zeros(slots),
        ]
    )
    re[1, 0] = im[1, 0] = 0.0
    re[3, 0] = RHO / STEPS
    im[:, 0] = [-RHO, 0.0, (gamma * (-1.0) ** n).sum(), -RHO / STEPS, 1.0]
    rows = np.concatenate([re.reshape(5, GROUPS, SLOTS), im.reshape(5, GROUPS, SLOTS)], axis=2)
    rows = rows.transpose(1, 0, 2)[..., None]
    return np.ascontiguousarray(np.broadcast_to(rows, (GROUPS, 5, 8, 128))).astype(np.float32)


def unit_of(j, imaginary):
    if j == STEPS // 2:
        j, imaginary = 0, True
    return (j // SLOTS) * 8 + (SLOTS if imaginary else 0) + j % SLOTS


def device_at(m, zz):
    r, along = lax.rem(m, 4), lax.div(m, 4)
    x = r + lax.rem(along, 2) * (3 - 2 * r)
    return (
        lax.rem(x, 2) * 16 + along * 2 + lax.rem(zz + m + 2, 2),
        lax.div(zz, 2) * 2 + lax.div(x, 2),
    )


def kernel(
    forcing,
    initial,
    coupling,
    velocity,
    table_in,
    out,
    slab,
    params,
    table,
    packed,
    times,
    spread,
    back,
    gathered,
    pack_params,
    own_params,
    near,
    coef,
    diag,
    d,
    middle_d,
    total,
    wrap,
    load_sem,
    out_send,
    out_recv,
    back_send,
    back_recv,
    param_send,
    param_recv,
    near_send,
    near_recv,
    halo_send,
    halo_recv,
):
    me_t, me_s = lax.axis_index("tm"), lax.axis_index("space")
    core, along = lax.rem(me_t, 2), lax.rem(lax.div(me_t, 2), 8)
    row, x_hi = lax.div(me_s, 2), lax.rem(me_s, 2)
    x = 2 * x_hi + lax.div(me_t, 16)
    r = x + lax.rem(along, 2) * (3 - 2 * x)
    m = along * 4 + r
    half = lax.rem(core + m, 2)
    zz = row * 2 + half
    swap = lax.rem(half + x_hi, 2)
    target = m + swap * (3 - 2 * r)
    x_lo = x - 2 * x_hi

    far_first = (4, 3, 5, 2, 6, 1, 7, 0)
    zs, turned = [None] * 8, [None] * 8
    odd_z = lax.rem(along, 2)
    for step in range(8):
        zs[step] = along + step - 8 * (along + step >= 8).astype(jnp.int32)
        turned[step] = 1 - odd_z if step % 2 else odd_z
    xs = [x + step - 4 * (x + step >= 4).astype(jnp.int32) for step in range(4)]
    x_his = [(v >= 2).astype(jnp.int32) for v in xs]

    loads = [
        pltpu.make_async_copy(forcing, slab, load_sem.at[0]),
        pltpu.make_async_copy(table_in, table, load_sem.at[1]),
    ]
    window = pl.ds(pl.multiple_of(lax.div(target, 2) * 8, 8), 8)
    param_loads = [
        pltpu.make_async_copy(coupling.at[:, window], params.at[0], load_sem.at[2]),
        pltpu.make_async_copy(velocity.at[:, :, window], params.at[pl.ds(1, 3)], load_sem.at[3]),
        pltpu.make_async_copy(initial.at[:, window], params.at[4], load_sem.at[4]),
    ]
    for load in loads + param_loads:
        load.start()

    barrier = pltpu.get_barrier_semaphore()

    sides = [(-1, 0), (1, 0), (0, -1), (0, 1), (-1, -1), (1, 1), (-1, 1), (1, -1)]
    opposite = [1, 0, 3, 2, 5, 4, 7, 6]
    in_y = {-1: m > 0, 1: m < 31}
    in_z = {-1: zz > 0, 1: zz < 7}
    side_device, has = [], []
    for by, bz in sides:
        side_device.append(device_at(m + by, zz + bz))
        inside = in_y[by] if by else in_z[bz]
        has.append(jnp.logical_and(in_y[by], in_z[bz]) if by and bz else inside)
    interior = jnp.logical_and(jnp.logical_and(has[0], has[1]), jnp.logical_and(has[2], has[3]))

    @pl.when(jnp.logical_not(interior))
    def _():
        zeros = jnp.zeros((8, 128), F32)
        for g in range(GROUPS):
            for parity in range(2):
                for z in range(8):
                    for y in range(8):
                        away = max(2 - z, z - 5, 0) + max(2 - y, y - 5, 0)
                        if 0 < away <= 2:
                            d[g, parity, z, y] = zeros
        near[...] = jnp.zeros_like(near)

    count = 31 + swap
    def senders():
        for step in far_first:
            for flip_x in range(2):
                for flip_core in range(2):
                    to_x = 1 - x_lo if flip_x else x_lo
                    to_core = 1 - core if flip_core else core
                    t = to_x * 16 + zs[step] * 2 + to_core
                    yield t, step == 0 and flip_x == 0 and flip_core == 0

    for t, mine in senders():

        @pl.when(swap == 1 if mine else True)
        def _():
            pl.semaphore_signal(barrier, inc=1, device_id=(t, row * 2 + half), device_id_type=MESH)

    for side in range(8):

        @pl.when(has[side])
        def _():
            pl.semaphore_signal(barrier, inc=1, device_id=side_device[side], device_id_type=MESH)

        count += has[side].astype(jnp.int32)

    low = lax.broadcasted_iota(jnp.int32, (8, 128), 0) < 4
    loads[0].wait()

    def pack(t, carry):
        rows = pl.ds(pl.multiple_of(t * 8, 8), 8)
        v = [slab[z, rows] for z in range(4)]
        w = [pltpu.roll(a, 4, 0) for a in v]
        packed[2 * t, 0:8] = jnp.where(low, v[0], w[1])
        packed[2 * t, 8:16] = jnp.where(low, v[2], w[3])
        packed[2 * t + 1, 0:8] = jnp.where(low, w[0], v[1])
        packed[2 * t + 1, 8:16] = jnp.where(low, w[2], v[3])
        return carry

    lax.fori_loop(0, 16, pack, 0)
    pl.semaphore_wait(barrier, count)

    for step in far_first:
        for to_x in range(4):
            chunk = 4 * zs[step] + xs[to_x] + turned[step] * (3 - 2 * xs[to_x])
            to = (
                (xs[to_x] - 2 * x_his[to_x]) * 16 + zs[step] * 2 + lax.rem(x_hi + chunk, 2),
                row * 2 + x_his[to_x],
            )

            @pl.when(swap == 1 if step == 0 and to_x == 0 else True)
            def _():
                pltpu.make_async_remote_copy(
                    src_ref=packed.at[chunk],
                    dst_ref=times.at[me_t],
                    send_sem=out_send,
                    recv_sem=out_recv,
                    device_id=to,
                    device_id_type=MESH,
                ).start()

    @pl.when(swap == 0)
    def _():
        times[me_t] = packed[m]

    def finish(src, dst, send_sem, recv_sem):
        for copies in range(2):

            @pl.when(swap == copies)
            def _():
                some = pl.ds(0, 31 + copies)
                pltpu.make_async_remote_copy(
                    src_ref=src.at[some],
                    dst_ref=dst.at[some],
                    send_sem=send_sem,
                    recv_sem=recv_sem,
                    device_id=(me_t, me_s),
                    device_id_type=MESH,
                ).wait()

    for load in param_loads:
        load.wait()
    odd = lax.rem(target, 2) == 1
    for f in range(5):
        v = [params[f, z] for z in range(4)]
        w = [pltpu.roll(a, 4, 0) for a in v]
        v, w = [jnp.where(odd, b, a) for a, b in zip(v, w)], [jnp.where(odd, a, b) for a, b in zip(v, w)]
        pack_params[f, 0:8] = jnp.where(low, v[0], w[1])
        pack_params[f, 8:16] = jnp.where(low, v[2], w[3])
    param_copy = pltpu.make_async_remote_copy(
        src_ref=pack_params,
        dst_ref=own_params,
        send_sem=param_send,
        recv_sem=param_recv,
        device_id=device_at(target, row * 2 + 1 - half),
        device_id_type=MESH,
    )
    @pl.when(swap == 1)
    def _():
        param_copy.start()
        param_copy.wait()

    @pl.when(swap == 0)
    def _():
        own_params[...] = pack_params[...]

    def near_copy(side):
        return pltpu.make_async_remote_copy(
            src_ref=own_params,
            dst_ref=near.at[side],
            send_sem=near_send.at[side],
            recv_sem=near_recv.at[side],
            device_id=side_device[side],
            device_id_type=MESH,
        )

    for side in range(4):

        @pl.when(has[side])
        def _():
            near_copy(side).start()

    lane = lax.broadcasted_iota(jnp.int32, (16, 128), 1)
    sub = lax.broadcasted_iota(jnp.int32, (16, 128), 0)
    loads[1].wait()

    def coefficients(ref):
        c = ref[0]
        flow = [c * ref[1 + k] for k in range(3)]
        return c, [
            c - flow[0],
            c + flow[0],
            c - flow[1],
            c + flow[1],
            jnp.where(lane == 127, 0.0, c - flow[2]),
            jnp.where(lane == 0, 0.0, c + flow[2]),
        ]

    def spread_coefficients(c, coefs, cells):
        middle = 1.0 + 6.0 * c
        for p, at in cells:
            for k in range(6):
                coef[at, k] = jnp.broadcast_to(coefs[k][p : p + 1], (8, 128))
            mid = jnp.broadcast_to(middle[p : p + 1], (8, 128))
            for g in range(GROUPS):
                d_re, d_im = mid - table[g, 0], table[g, 1]
                inv = 1.0 / (d_re * d_re + d_im * d_im)
                diag[g, at, 0] = d_re * inv
                diag[g, at, 1] = d_im * inv

    c, coefs = coefficients(own_params)
    spread_coefficients(c, coefs, [(p, p) for p in range(16)])
    for side in range(4):

        @pl.when(has[side])
        def _():
            near_copy(side).wait_send()

        @pl.when(has[opposite[side]])
        def _():
            near_copy(side).wait_recv()

    ring_rows = [[4 * i for i in range(4)], [4 * i + 3 for i in range(4)], range(4), range(12, 16)]
    for side in range(4):
        cells = [(p, 16 + side * 4 + i) for i, p in enumerate(ring_rows[side])]
        spread_coefficients(*coefficients(near.at[side]), cells)
    own = own_params[4]
    after_y, before_y, after_z, before_z = [near[side, 4] for side in range(4)]
    step = lax.rem(sub, 4)
    summed = coefs[0] * jnp.where(sub < 12, pltpu.roll(own, 12, 0), pltpu.roll(after_z, 12, 0))
    summed += coefs[1] * jnp.where(sub >= 4, pltpu.roll(own, 4, 0), pltpu.roll(before_z, 4, 0))
    summed += coefs[2] * jnp.where(step < 3, pltpu.roll(own, 15, 0), pltpu.roll(after_y, 3, 0))
    summed += coefs[3] * jnp.where(step > 0, pltpu.roll(own, 1, 0), pltpu.roll(before_y, 13, 0))
    summed += coefs[4] * pltpu.roll(own, 127, 1) + coefs[5] * pltpu.roll(own, 1, 1)
    source = summed - 6.0 * c * own

    finish(packed, times, out_send, out_recv)

    def transform(h, carry):
        rows = pl.ds(pl.multiple_of(h * 8, 8), 8)
        re, im = real_fft([GAMMA[n] * times[n, rows] for n in range(32)])
        for j in range(17):
            spread[pl.ds(h * 256 + unit_of(j, False), 8, stride=32), :] = re[j]
            if im[j] is not None:
                spread[pl.ds(h * 256 + unit_of(j, True), 8, stride=32), :] = im[j]
        return carry

    lax.fori_loop(0, 2, transform, 0)

    def halo_copy(g, parity, side):
        refs = []
        for shift in (0, 4):
            at = []
            for by, bz in ((sides[side][1], sides[side][0]), (sides[side][0], sides[side][1])):
                if by == 0:
                    at.append(pl.ds(2, 4))
                elif bz == 0:
                    at.append(pl.ds((2 if by < 0 else 4) - by * shift, 2))
                else:
                    at.append((2 if by < 0 else 5) - by * shift)
            refs.append(d.at[g, parity, at[0], at[1]])
        return pltpu.make_async_remote_copy(
            src_ref=refs[0],
            dst_ref=refs[1],
            send_sem=halo_send.at[g, parity, side // 4],
            recv_sem=halo_recv.at[g, parity, side // 4],
            device_id=side_device[side],
            device_id_type=MESH,
        )

    corners_first = (4, 5, 6, 7, 0, 1, 2, 3)

    def halo_start(g, parity):
        @pl.when(interior)
        def _():
            for side in corners_first:
                halo_copy(g, parity, side).start()

        @pl.when(jnp.logical_not(interior))
        def _():
            for side in corners_first:

                @pl.when(has[side])
                def _():
                    halo_copy(g, parity, side).start()

    whole_y, whole_z = jnp.logical_and(has[0], has[1]), jnp.logical_and(has[2], has[3])

    def halo_wait(g, parity, corners):
        for tiles, when in (
            ((32, 4), interior),
            ((24, 2), whole_y != whole_z),
            ((16, 1), jnp.logical_not(jnp.logical_or(whole_y, whole_z))),
        ):

            @pl.when(when)
            def _():
                amount = spread.at[pl.ds(0, tiles[corners] * 8)]
                pltpu.make_async_remote_copy(
                    src_ref=amount,
                    dst_ref=amount,
                    send_sem=halo_send.at[g, parity, corners],
                    recv_sem=halo_recv.at[g, parity, corners],
                    device_id=(me_t, me_s),
                    device_id_type=MESH,
                ).wait()

    def divide(g, at, s):
        return diag[g, at, 0] * s + diag[g, at, 1] * pltpu.roll(s, 4, 0)

    def stencil(field, z, y, at):
        here = field[z, y]
        s = coef[at, 0] * field[z + 1, y]
        s += coef[at, 1] * field[z - 1, y]
        s += coef[at, 2] * field[z, y + 1]
        s += coef[at, 3] * field[z, y - 1]
        s += coef[at, 4] * pltpu.roll(here, 127, 1)
        s += coef[at, 5] * pltpu.roll(here, 1, 1)
        return s

    for g in range(GROUPS):
        for p in range(16):
            z, y = p // 4, p % 4
            base = jnp.broadcast_to(source[p : p + 1], (8, 128))
            rows = pl.ds(p * 32 + g * 8, 8)
            v = divide(g, p, spread[rows] + table[g, 2] * base)
            d[g, 0, z + 2, y + 2] = v
            total[rows] = v
        halo_start(g, 0)

    ring = [(i, -1) for i in range(4)] + [(i, 4) for i in range(4)]
    ring = ring + [(-1, i) for i in range(4)] + [(4, i) for i in range(4)]
    ring = ring[4:8] + ring[0:4] + ring[12:16] + ring[8:12]

    plain = [16 + i for i in range(16) if i % 4 in (1, 2)]
    beside = [16 + i for i in range(16) if i % 4 in (0, 3)]

    def two_sweeps(g, parity, send):
        old, new = d.at[g, parity], d.at[g, 1 - parity]
        halo_wait(g, parity, 0)
        for cells in (list(range(16)) + plain, beside):
            if cells is beside:
                halo_wait(g, parity, 1)
            for at in cells:
                z, y = (at // 4, at % 4) if at < 16 else ring[at - 16]
                v = divide(g, at, stencil(old, z + 2, y + 2, at))
                middle_d[z + 1, y + 1] = v
                if at < 16:
                    total[pl.ds(at * 32 + g * 8, 8)] += v
        for at in range(16):
            z, y = at // 4, at % 4
            v = divide(g, at, stencil(middle_d, z + 1, y + 1, at))
            new[z + 2, y + 2] = v
            total[pl.ds(at * 32 + g * 8, 8)] += v
        if send:
            halo_start(g, 1 - parity)

    def all_groups(k, carry):
        for g in range(GROUPS):
            two_sweeps(g, lax.rem(k, 2), True)
        return carry

    lax.fori_loop(0, 4, all_groups, 0)
    for p in range(16):
        s = jnp.zeros((8, 128), F32)
        for g in range(GROUPS):
            s += table[g, 3] * total[pl.ds(p * 32 + g * 8, 8)]
        wrap[p] = jnp.broadcast_to(jnp.sum(s, axis=0, keepdims=True), (8, 128))
    for g in range(GROUPS):
        halo_wait(g, 0, 0)
        halo_wait(g, 0, 1)
        for at in range(16):
            z, y = at // 4, at % 4
            s = stencil(d.at[g, 0], z + 2, y + 2, at) - table[g, 4] * wrap[at]
            v = divide(g, at, s)
            d[g, 1, z + 2, y + 2] = v
            total[pl.ds(at * 32 + g * 8, 8)] += v
        halo_start(g, 1)
    lax.fori_loop(5, 8, all_groups, 0)
    for g in range(GROUPS):
        two_sweeps(g, 0, False)

    def restore(h, carry):
        rows = pl.ds(pl.multiple_of(h * 8, 8), 8)
        re, im = [None] * 17, [None] * 17
        for j in range(17):
            re[j] = total[pl.ds(h * 256 + unit_of(j, False), 8, stride=32), :]
            if 0 < j < 16:
                im[j] = total[pl.ds(h * 256 + unit_of(j, True), 8, stride=32), :]
        for n, value in enumerate(real_ifft(re, im)):
            back[n, rows] = value * (1.0 / (STEPS * GAMMA[n]))
        return carry

    lax.fori_loop(0, 2, restore, 0)

    for t, mine in senders():

        @pl.when(swap == 1 if mine else True)
        def _():
            pltpu.make_async_remote_copy(
                src_ref=back.at[t],
                dst_ref=gathered.at[m],
                send_sem=back_send,
                recv_sem=back_recv,
                device_id=(t, row * 2 + half),
                device_id_type=MESH,
            ).start()

    @pl.when(swap == 0)
    def _():
        gathered[m] = back[me_t]

    finish(back, gathered, back_send, back_recv)

    def unpack(t, carry):
        rows = pl.ds(pl.multiple_of(t * 8, 8), 8)
        p = [gathered[2 * t, 0:8], gathered[2 * t, 8:16]]
        q = [gathered[2 * t + 1, 0:8], gathered[2 * t + 1, 8:16]]
        for i in range(2):
            out[2 * i, rows] = jnp.where(low, p[i], pltpu.roll(q[i], 4, 0))
            out[2 * i + 1, rows] = jnp.where(low, pltpu.roll(p[i], 4, 0), q[i])
        return carry

    lax.fori_loop(0, 16, unpack, 0)


def body(forcing, initial, coupling, velocity):
    local = forcing.shape[1:]
    table = jnp.asarray(unit_tables())
    hbm = pl.BlockSpec(memory_space=pl.ANY)
    dma = pltpu.SemaphoreType.DMA
    correction = pl.pallas_call(
        kernel,
        out_shape=pltpu.VMEM(local, F32),
        in_specs=[hbm] * 5,
        out_specs=pl.BlockSpec(memory_space=pltpu.VMEM),
        scratch_shapes=[
            pltpu.VMEM(local, F32),
            pltpu.VMEM((5, 4, 8, 128), F32),
            pltpu.VMEM((GROUPS, 5, 8, 128), F32),
            pltpu.VMEM((32, 16, 128), F32),
            pltpu.VMEM((32, 16, 128), F32),
            pltpu.VMEM((512, 128), F32),
            pltpu.VMEM((32, 16, 128), F32),
            pltpu.VMEM((32, 16, 128), F32),
            pltpu.VMEM((5, 16, 128), F32),
            pltpu.VMEM((5, 16, 128), F32),
            pltpu.VMEM((4, 5, 16, 128), F32),
            pltpu.VMEM((32, 6, 8, 128), F32),
            pltpu.VMEM((GROUPS, 32, 2, 8, 128), F32),
            pltpu.VMEM((GROUPS, 2, 8, 8, 8, 128), F32),
            pltpu.VMEM((6, 6, 8, 128), F32),
            pltpu.VMEM((512, 128), F32),
            pltpu.VMEM((16, 8, 128), F32),
            dma((5,)),
            dma,
            dma,
            dma,
            dma,
            dma,
            dma,
            dma((4,)),
            dma((4,)),
            dma((GROUPS, 2, 2)),
            dma((GROUPS, 2, 2)),
        ],
        compiler_params=pltpu.CompilerParams(collective_id=0, has_side_effects=True),
    )(forcing[0], initial, coupling, velocity, table)
    return (initial + correction)[None]


def solution(mesh):
    return jax.shard_map(
        body,
        mesh=mesh,
        in_specs=(
            P("tm", "space", None, None),
            P("space", None, None),
            P("space", None, None),
            P(None, "space", None, None),
        ),
        out_specs=P("tm", "space", None, None),
        check_vma=False,
    )
```

```python
import functools
import math

import jax
import jax.numpy as jnp
import numpy as np
from jax import lax
from jax.experimental import pallas as pl
from jax.experimental.pallas import tpu as pltpu
from jax.sharding import PartitionSpec as P

STEPS = 32
ALPHA = 0.1
RHO = ALPHA ** (1.0 / STEPS)
GAMMA = [ALPHA ** (n / STEPS) for n in range(STEPS)]
GROUPS = 4
SLOTS = STEPS // 2 // GROUPS
MESH = pl.DeviceIdType.MESH
F32 = jnp.float32


def real_fft(xs):
    size = len(xs)
    if size == 2:
        return [xs[0] + xs[1], xs[0] - xs[1]], [None, None]
    even_re, even_im = real_fft(xs[0::2])
    odd_re, odd_im = real_fft(xs[1::2])
    half, quarter = size // 2, size // 4
    re, im = [None] * (half + 1), [None] * (half + 1)
    re[0], re[half] = even_re[0] + odd_re[0], even_re[0] - odd_re[0]
    for j in range(1, quarter):
        c, s = math.cos(2 * math.pi * j / size), math.sin(2 * math.pi * j / size)
        t_re = c * odd_re[j] + s * odd_im[j]
        t_im = c * odd_im[j] - s * odd_re[j]
        re[j], im[j] = even_re[j] + t_re, even_im[j] + t_im
        re[half - j], im[half - j] = even_re[j] - t_re, t_im - even_im[j]
    re[quarter], im[quarter] = even_re[quarter], -odd_re[quarter]
    return re, im


def real_ifft(re, im):
    half = len(re) - 1
    size = 2 * half
    if size == 2:
        return [re[0] + re[1], re[0] - re[1]]
    quarter = size // 4
    even_re, even_im = [None] * (quarter + 1), [None] * (quarter + 1)
    odd_re, odd_im = [None] * (quarter + 1), [None] * (quarter + 1)
    even_re[0], odd_re[0] = re[0] + re[half], re[0] - re[half]
    for j in range(1, quarter):
        c, s = math.cos(2 * math.pi * j / size), math.sin(2 * math.pi * j / size)
        even_re[j], even_im[j] = re[j] + re[half - j], im[j] - im[half - j]
        t_re, t_im = re[j] - re[half - j], im[j] + im[half - j]
        odd_re[j], odd_im[j] = c * t_re - s * t_im, c * t_im + s * t_re
    even_re[quarter], odd_re[quarter] = 2.0 * re[quarter], -2.0 * im[quarter]
    even = real_ifft(even_re, even_im)
    odd = real_ifft(odd_re, odd_im)
    return [(even, odd)[n % 2][n // 2] for n in range(size)]


def unit_tables():
    slots = STEPS // 2
    j = np.arange(slots)
    theta = 2 * np.pi * j / STEPS
    n = np.arange(STEPS)
    gamma = np.array(GAMMA)
    angle = 2 * np.pi * ((j[:, None] * n[None, :]) % STEPS) / STEPS
    last = 2 * np.pi * ((j * (STEPS - 1)) % STEPS) / STEPS
    re = np.stack(
        [
            RHO * np.cos(theta),
            RHO * np.sin(theta),
            (np.cos(angle) * gamma).sum(1),
            2 * np.cos(last) * RHO / STEPS,
            np.ones(slots),
        ]
    )
    im = np.stack(
        [
            RHO * np.cos(theta),
            -RHO * np.sin(theta),
            -(np.sin(angle) * gamma).sum(1),
            -2 * np.sin(last) * RHO / STEPS,
            np.zeros(slots),
        ]
    )
    re[1, 0] = im[1, 0] = 0.0
    re[3, 0] = RHO / STEPS
    im[:, 0] = [-RHO, 0.0, (gamma * (-1.0) ** n).sum(), -RHO / STEPS, 1.0]
    rows = np.concatenate([re.reshape(5, GROUPS, SLOTS), im.reshape(5, GROUPS, SLOTS)], axis=2)
    rows = rows.transpose(1, 0, 2)[..., None]
    return np.ascontiguousarray(np.broadcast_to(rows, (GROUPS, 5, 8, 128))).astype(np.float32)


def unit_of(j, imaginary):
    if j == STEPS // 2:
        j, imaginary = 0, True
    return (j // SLOTS) * 8 + (SLOTS if imaginary else 0) + j % SLOTS


def device_at(m, zz):
    r, along = lax.rem(m, 4), lax.div(m, 4)
    x = r + lax.rem(along, 2) * (3 - 2 * r)
    return (
        lax.rem(x, 2) * 16 + along * 2 + lax.rem(zz + m + 2, 2),
        lax.div(zz, 2) * 2 + lax.div(x, 2),
    )


def kernel(
    forcing,
    initial,
    coupling,
    velocity,
    table_in,
    out,
    slab,
    params,
    table,
    packed,
    times,
    spread,
    back,
    gathered,
    pack_params,
    own_params,
    near,
    coef,
    diag,
    d,
    middle_d,
    total,
    wrap,
    load_sem,
    out_send,
    out_recv,
    back_send,
    back_recv,
    param_send,
    param_recv,
    near_send,
    near_recv,
    halo_send,
    halo_recv,
):
    me_t, me_s = lax.axis_index("tm"), lax.axis_index("space")
    core, along = lax.rem(me_t, 2), lax.rem(lax.div(me_t, 2), 8)
    row, x_hi = lax.div(me_s, 2), lax.rem(me_s, 2)
    x = 2 * x_hi + lax.div(me_t, 16)
    r = x + lax.rem(along, 2) * (3 - 2 * x)
    m = along * 4 + r
    half = lax.rem(core + m, 2)
    zz = row * 2 + half
    swap = lax.rem(half + x_hi, 2)
    target = m + swap * (3 - 2 * r)
    x_lo = x - 2 * x_hi

    far_first = (4, 3, 5, 2, 6, 1, 7, 0)
    zs, turned = [None] * 8, [None] * 8
    odd_z = lax.rem(along, 2)
    for step in range(8):
        zs[step] = along + step - 8 * (along + step >= 8).astype(jnp.int32)
        turned[step] = 1 - odd_z if step % 2 else odd_z
    xs = [x + step - 4 * (x + step >= 4).astype(jnp.int32) for step in range(4)]
    x_his = [(v >= 2).astype(jnp.int32) for v in xs]

    loads = [
        pltpu.make_async_copy(forcing, slab, load_sem.at[0]),
        pltpu.make_async_copy(table_in, table, load_sem.at[1]),
    ]
    window = pl.ds(pl.multiple_of(lax.div(target, 2) * 8, 8), 8)
    param_loads = [
        pltpu.make_async_copy(coupling.at[:, window], params.at[0], load_sem.at[2]),
        pltpu.make_async_copy(velocity.at[:, :, window], params.at[pl.ds(1, 3)], load_sem.at[3]),
        pltpu.make_async_copy(initial.at[:, window], params.at[4], load_sem.at[4]),
    ]
    for load in loads + param_loads:
        load.start()

    barrier = pltpu.get_barrier_semaphore()

    sides = [(-1, 0), (1, 0), (0, -1), (0, 1), (-1, -1), (1, 1), (-1, 1), (1, -1)]
    opposite = [1, 0, 3, 2, 5, 4, 7, 6]
    in_y = {-1: m > 0, 1: m < 31}
    in_z = {-1: zz > 0, 1: zz < 7}
    side_device, has = [], []
    for by, bz in sides:
        side_device.append(device_at(m + by, zz + bz))
        inside = in_y[by] if by else in_z[bz]
        has.append(jnp.logical_and(in_y[by], in_z[bz]) if by and bz else inside)
    interior = jnp.logical_and(jnp.logical_and(has[0], has[1]), jnp.logical_and(has[2], has[3]))

    @pl.when(jnp.logical_not(interior))
    def _():
        zeros = jnp.zeros((8, 128), F32)
        for g in range(GROUPS):
            for parity in range(2):
                for z in range(8):
                    for y in range(8):
                        away = max(2 - z, z - 5, 0) + max(2 - y, y - 5, 0)
                        if 0 < away <= 2:
                            d[g, parity, z, y] = zeros
        near[...] = jnp.zeros_like(near)

    count = 31 + swap
    def senders():
        order = [(step, near) for step in far_first for near in range(2)]
        for step, near in sorted(order, key=lambda at: at[1] - min(at[0], 8 - at[0])):
            flip = swap if near else 1 - swap
            to_x = x_lo + flip - 2 * x_lo * flip
            for to_core in (1 - core, core):
                mine = step == 0 and near == 1 and to_core is core
                yield to_x * 16 + zs[step] * 2 + to_core, mine

    for t, mine in senders():

        @pl.when(swap == 1 if mine else True)
        def _():
            pl.semaphore_signal(barrier, inc=1, device_id=(t, row * 2 + half), device_id_type=MESH)

    for side in range(8):

        @pl.when(has[side])
        def _():
            pl.semaphore_signal(barrier, inc=1, device_id=side_device[side], device_id_type=MESH)

        count += has[side].astype(jnp.int32)

    low = lax.broadcasted_iota(jnp.int32, (8, 128), 0) < 4
    loads[0].wait()

    def pack(t, carry):
        rows = pl.ds(pl.multiple_of(t * 8, 8), 8)
        v = [slab[z, rows] for z in range(4)]
        w = [pltpu.roll(a, 4, 0) for a in v]
        packed[2 * t, 0:8] = jnp.where(low, v[0], w[1])
        packed[2 * t, 8:16] = jnp.where(low, v[2], w[3])
        packed[2 * t + 1, 0:8] = jnp.where(low, w[0], v[1])
        packed[2 * t + 1, 8:16] = jnp.where(low, w[2], v[3])
        return carry

    lax.fori_loop(0, 16, pack, 0)
    pl.semaphore_wait(barrier, count)

    for step in far_first:
        for to_x in range(4):
            chunk = 4 * zs[step] + xs[to_x] + turned[step] * (3 - 2 * xs[to_x])
            to = (
                (xs[to_x] - 2 * x_his[to_x]) * 16 + zs[step] * 2 + lax.rem(x_hi + chunk, 2),
                row * 2 + x_his[to_x],
            )

            @pl.when(swap == 1 if step == 0 and to_x == 0 else True)
            def _():
                pltpu.make_async_remote_copy(
                    src_ref=packed.at[chunk],
                    dst_ref=times.at[me_t],
                    send_sem=out_send,
                    recv_sem=out_recv,
                    device_id=to,
                    device_id_type=MESH,
                ).start()

    @pl.when(swap == 0)
    def _():
        times[me_t] = packed[m]

    def finish(src, dst, send_sem, recv_sem):
        for copies in range(2):

            @pl.when(swap == copies)
            def _():
                some = pl.ds(0, 31 + copies)
                pltpu.make_async_remote_copy(
                    src_ref=src.at[some],
                    dst_ref=dst.at[some],
                    send_sem=send_sem,
                    recv_sem=recv_sem,
                    device_id=(me_t, me_s),
                    device_id_type=MESH,
                ).wait()

    for load in param_loads:
        load.wait()
    odd = lax.rem(target, 2) == 1
    for f in range(5):
        v = [params[f, z] for z in range(4)]
        w = [pltpu.roll(a, 4, 0) for a in v]
        v, w = [jnp.where(odd, b, a) for a, b in zip(v, w)], [jnp.where(odd, a, b) for a, b in zip(v, w)]
        pack_params[f, 0:8] = jnp.where(low, v[0], w[1])
        pack_params[f, 8:16] = jnp.where(low, v[2], w[3])
    param_copy = pltpu.make_async_remote_copy(
        src_ref=pack_params,
        dst_ref=own_params,
        send_sem=param_send,
        recv_sem=param_recv,
        device_id=device_at(target, row * 2 + 1 - half),
        device_id_type=MESH,
    )
    @pl.when(swap == 1)
    def _():
        param_copy.start()
        param_copy.wait()

    @pl.when(swap == 0)
    def _():
        own_params[...] = pack_params[...]

    def near_copy(side):
        return pltpu.make_async_remote_copy(
            src_ref=own_params,
            dst_ref=near.at[side],
            send_sem=near_send.at[side],
            recv_sem=near_recv.at[side],
            device_id=side_device[side],
            device_id_type=MESH,
        )

    for side in range(4):

        @pl.when(has[side])
        def _():
            near_copy(side).start()

    lane = lax.broadcasted_iota(jnp.int32, (16, 128), 1)
    sub = lax.broadcasted_iota(jnp.int32, (16, 128), 0)
    loads[1].wait()

    def coefficients(ref):
        c = ref[0]
        flow = [c * ref[1 + k] for k in range(3)]
        return c, [
            c - flow[0],
            c + flow[0],
            c - flow[1],
            c + flow[1],
            jnp.where(lane == 127, 0.0, c - flow[2]),
            jnp.where(lane == 0, 0.0, c + flow[2]),
        ]

    def spread_coefficients(c, coefs, cells):
        middle = 1.0 + 6.0 * c
        for p, at in cells:
            for k in range(6):
                coef[at, k] = jnp.broadcast_to(coefs[k][p : p + 1], (8, 128))
            mid = jnp.broadcast_to(middle[p : p + 1], (8, 128))
            for g in range(GROUPS):
                d_re, d_im = mid - table[g, 0], table[g, 1]
                inv = 1.0 / (d_re * d_re + d_im * d_im)
                diag[g, at, 0] = d_re * inv
                diag[g, at, 1] = d_im * inv

    c, coefs = coefficients(own_params)
    spread_coefficients(c, coefs, [(p, p) for p in range(16)])
    for side in range(4):

        @pl.when(has[side])
        def _():
            near_copy(side).wait_send()

        @pl.when(has[opposite[side]])
        def _():
            near_copy(side).wait_recv()

    ring_rows = [[4 * i for i in range(4)], [4 * i + 3 for i in range(4)], range(4), range(12, 16)]
    for side in range(4):
        cells = [(p, 16 + side * 4 + i) for i, p in enumerate(ring_rows[side])]
        spread_coefficients(*coefficients(near.at[side]), cells)
    own = own_params[4]
    after_y, before_y, after_z, before_z = [near[side, 4] for side in range(4)]
    step = lax.rem(sub, 4)
    summed = coefs[0] * jnp.where(sub < 12, pltpu.roll(own, 12, 0), pltpu.roll(after_z, 12, 0))
    summed += coefs[1] * jnp.where(sub >= 4, pltpu.roll(own, 4, 0), pltpu.roll(before_z, 4, 0))
    summed += coefs[2] * jnp.where(step < 3, pltpu.roll(own, 15, 0), pltpu.roll(after_y, 3, 0))
    summed += coefs[3] * jnp.where(step > 0, pltpu.roll(own, 1, 0), pltpu.roll(before_y, 13, 0))
    summed += coefs[4] * pltpu.roll(own, 127, 1) + coefs[5] * pltpu.roll(own, 1, 1)
    source = summed - 6.0 * c * own

    finish(packed, times, out_send, out_recv)

    def transform(h, carry):
        rows = pl.ds(pl.multiple_of(h * 8, 8), 8)
        re, im = real_fft([GAMMA[n] * times[n, rows] for n in range(32)])
        for j in range(17):
            spread[pl.ds(h * 256 + unit_of(j, False), 8, stride=32), :] = re[j]
            if im[j] is not None:
                spread[pl.ds(h * 256 + unit_of(j, True), 8, stride=32), :] = im[j]
        return carry

    lax.fori_loop(0, 2, transform, 0)

    def halo_copy(g, parity, side):
        refs = []
        for shift in (0, 4):
            at = []
            for by, bz in ((sides[side][1], sides[side][0]), (sides[side][0], sides[side][1])):
                if by == 0:
                    at.append(pl.ds(2, 4))
                elif bz == 0:
                    at.append(pl.ds((2 if by < 0 else 4) - by * shift, 2))
                else:
                    at.append((2 if by < 0 else 5) - by * shift)
            refs.append(d.at[g, parity, at[0], at[1]])
        return pltpu.make_async_remote_copy(
            src_ref=refs[0],
            dst_ref=refs[1],
            send_sem=halo_send.at[g, parity, side // 4],
            recv_sem=halo_recv.at[g, parity, side // 4],
            device_id=side_device[side],
            device_id_type=MESH,
        )

    corners_first = (4, 5, 6, 7, 0, 1, 2, 3)

    def halo_start(g, parity):
        @pl.when(interior)
        def _():
            for side in corners_first:
                halo_copy(g, parity, side).start()

        @pl.when(jnp.logical_not(interior))
        def _():
            for side in corners_first:

                @pl.when(has[side])
                def _():
                    halo_copy(g, parity, side).start()

    whole_y, whole_z = jnp.logical_and(has[0], has[1]), jnp.logical_and(has[2], has[3])

    def halo_wait(g, parity, corners):
        for tiles, when in (
            ((32, 4), interior),
            ((24, 2), whole_y != whole_z),
            ((16, 1), jnp.logical_not(jnp.logical_or(whole_y, whole_z))),
        ):

            @pl.when(when)
            def _():
                amount = spread.at[pl.ds(0, tiles[corners] * 8)]
                pltpu.make_async_remote_copy(
                    src_ref=amount,
                    dst_ref=amount,
                    send_sem=halo_send.at[g, parity, corners],
                    recv_sem=halo_recv.at[g, parity, corners],
                    device_id=(me_t, me_s),
                    device_id_type=MESH,
                ).wait()

    def divide(g, at, s):
        return diag[g, at, 0] * s + diag[g, at, 1] * pltpu.roll(s, 4, 0)

    def stencil(field, z, y, at):
        here = field[z, y]
        s = coef[at, 0] * field[z + 1, y]
        s += coef[at, 1] * field[z - 1, y]
        s += coef[at, 2] * field[z, y + 1]
        s += coef[at, 3] * field[z, y - 1]
        s += coef[at, 4] * pltpu.roll(here, 127, 1)
        s += coef[at, 5] * pltpu.roll(here, 1, 1)
        return s

    for g in range(GROUPS):
        for p in range(16):
            z, y = p // 4, p % 4
            base = jnp.broadcast_to(source[p : p + 1], (8, 128))
            rows = pl.ds(p * 32 + g * 8, 8)
            v = divide(g, p, spread[rows] + table[g, 2] * base)
            d[g, 0, z + 2, y + 2] = v
            total[rows] = v
        halo_start(g, 0)

    ring = [(i, -1) for i in range(4)] + [(i, 4) for i in range(4)]
    ring = ring + [(-1, i) for i in range(4)] + [(4, i) for i in range(4)]
    ring = ring[4:8] + ring[0:4] + ring[12:16] + ring[8:12]

    plain = [16 + i for i in range(16) if i % 4 in (1, 2)]
    beside = [16 + i for i in range(16) if i % 4 in (0, 3)]

    def two_sweeps(g, parity, send):
        old, new = d.at[g, parity], d.at[g, 1 - parity]
        halo_wait(g, parity, 0)
        for cells in (list(range(16)) + plain, beside):
            if cells is beside:
                halo_wait(g, parity, 1)
            for at in cells:
                z, y = (at // 4, at % 4) if at < 16 else ring[at - 16]
                v = divide(g, at, stencil(old, z + 2, y + 2, at))
                middle_d[z + 1, y + 1] = v
                if at < 16:
                    total[pl.ds(at * 32 + g * 8, 8)] += v
        for at in range(16):
            z, y = at // 4, at % 4
            v = divide(g, at, stencil(middle_d, z + 1, y + 1, at))
            new[z + 2, y + 2] = v
            total[pl.ds(at * 32 + g * 8, 8)] += v
        if send:
            halo_start(g, 1 - parity)

    def all_groups(k, carry):
        for g in range(GROUPS):
            two_sweeps(g, lax.rem(k, 2), True)
        return carry

    lax.fori_loop(0, 4, all_groups, 0)
    for p in range(16):
        s = jnp.zeros((8, 128), F32)
        for g in range(GROUPS):
            s += table[g, 3] * total[pl.ds(p * 32 + g * 8, 8)]
        wrap[p] = jnp.broadcast_to(jnp.sum(s, axis=0, keepdims=True), (8, 128))
    for g in range(GROUPS):
        halo_wait(g, 0, 0)
        halo_wait(g, 0, 1)
        for at in range(16):
            z, y = at // 4, at % 4
            s = stencil(d.at[g, 0], z + 2, y + 2, at) - table[g, 4] * wrap[at]
            v = divide(g, at, s)
            d[g, 1, z + 2, y + 2] = v
            total[pl.ds(at * 32 + g * 8, 8)] += v
        halo_start(g, 1)
    lax.fori_loop(5, 8, all_groups, 0)
    for g in range(GROUPS):
        two_sweeps(g, 0, False)

    def restore(h, carry):
        rows = pl.ds(pl.multiple_of(h * 8, 8), 8)
        re, im = [None] * 17, [None] * 17
        for j in range(17):
            re[j] = total[pl.ds(h * 256 + unit_of(j, False), 8, stride=32), :]
            if 0 < j < 16:
                im[j] = total[pl.ds(h * 256 + unit_of(j, True), 8, stride=32), :]
        for n, value in enumerate(real_ifft(re, im)):
            back[n, rows] = value * (1.0 / (STEPS * GAMMA[n]))
        return carry

    lax.fori_loop(0, 2, restore, 0)

    for t, mine in senders():

        @pl.when(swap == 1 if mine else True)
        def _():
            pltpu.make_async_remote_copy(
                src_ref=back.at[t],
                dst_ref=gathered.at[m],
                send_sem=back_send,
                recv_sem=back_recv,
                device_id=(t, row * 2 + half),
                device_id_type=MESH,
            ).start()

    @pl.when(swap == 0)
    def _():
        gathered[m] = back[me_t]

    finish(back, gathered, back_send, back_recv)

    def unpack(t, carry):
        rows = pl.ds(pl.multiple_of(t * 8, 8), 8)
        p = [gathered[2 * t, 0:8], gathered[2 * t, 8:16]]
        q = [gathered[2 * t + 1, 0:8], gathered[2 * t + 1, 8:16]]
        for i in range(2):
            out[2 * i, rows] = jnp.where(low, p[i], pltpu.roll(q[i], 4, 0))
            out[2 * i + 1, rows] = jnp.where(low, pltpu.roll(p[i], 4, 0), q[i])
        return carry

    lax.fori_loop(0, 16, unpack, 0)


def body(forcing, initial, coupling, velocity):
    local = forcing.shape[1:]
    table = jnp.asarray(unit_tables())
    hbm = pl.BlockSpec(memory_space=pl.ANY)
    dma = pltpu.SemaphoreType.DMA
    correction = pl.pallas_call(
        kernel,
        out_shape=pltpu.VMEM(local, F32),
        in_specs=[hbm] * 5,
        out_specs=pl.BlockSpec(memory_space=pltpu.VMEM),
        scratch_shapes=[
            pltpu.VMEM(local, F32),
            pltpu.VMEM((5, 4, 8, 128), F32),
            pltpu.VMEM((GROUPS, 5, 8, 128), F32),
            pltpu.VMEM((32, 16, 128), F32),
            pltpu.VMEM((32, 16, 128), F32),
            pltpu.VMEM((512, 128), F32),
            pltpu.VMEM((32, 16, 128), F32),
            pltpu.VMEM((32, 16, 128), F32),
            pltpu.VMEM((5, 16, 128), F32),
            pltpu.VMEM((5, 16, 128), F32),
            pltpu.VMEM((4, 5, 16, 128), F32),
            pltpu.VMEM((32, 6, 8, 128), F32),
            pltpu.VMEM((GROUPS, 32, 2, 8, 128), F32),
            pltpu.VMEM((GROUPS, 2, 8, 8, 8, 128), F32),
            pltpu.VMEM((6, 6, 8, 128), F32),
            pltpu.VMEM((512, 128), F32),
            pltpu.VMEM((16, 8, 128), F32),
            dma((5,)),
            dma,
            dma,
            dma,
            dma,
            dma,
            dma,
            dma((4,)),
            dma((4,)),
            dma((GROUPS, 2, 2)),
            dma((GROUPS, 2, 2)),
        ],
        compiler_params=pltpu.CompilerParams(collective_id=0, has_side_effects=True),
    )(forcing[0], initial, coupling, velocity, table)
    return (initial + correction)[None]


def solution(mesh):
    return jax.shard_map(
        body,
        mesh=mesh,
        in_specs=(
            P("tm", "space", None, None),
            P("space", None, None),
            P("space", None, None),
            P(None, "space", None, None),
        ),
        out_specs=P("tm", "space", None, None),
        check_vma=False,
    )
```
